32 devices in a mesh: member: 8 (over y, x, core), space: 4 (over z).
Axes of the slice: x: 2, y: 2, z: 4, core: 2. Of those that a mesh axis runs over, the one named last changes fastest.
Arguments:
- ensemble: float32 [8, 3, 8, 48, 128], P('member', None, 'space')
- obs_cell: int32 [2048], P('space'), may hold values from 0 to 12287
- obs_comp: int32 [2048], P('space'), may hold values from 0 to 2
- obs_value: float32 [2048], replicated, may hold values from -6 to 6
- obs_precision: float32 [2048], replicated, may hold values from 0.3 to 5
- loc_obs: int32 [4096, 128], P(('space', 'member')), may hold values from 0 to 2047
- loc_level: int32 [4096, 128], P(('space', 'member')), may hold values from 1 to 8
Outputs:
- analysis: float32 [8, 3, 8, 48, 128], P('member', None, 'space')
The draws below stay inside these ranges and needn't reach their ends.
Inputs may be any that keep to these rules, and one draw needn't show every extreme that they name: Observation i lies in the slab of index i // 512; obs_cell is x' * 48 * 128 + y * 128 + z with x' counted within that slab.
All inputs are finite; a program needn't handle non-finite values.
Results may differ from the reference program's by a relative error of at most 0.0003.
Values sent between devices are 32-bit elements; how exact they have to be, the bound alone decides.
A program may use at most 64 MiB of HBM per device.

```python
import math
import jax
import jax.numpy as jnp
from jax import lax

CX = 2
NY = 48
NZ = 128
NOB_DEV = 512
LOC = 128
NS_ITERS = 8
LEVELS = 8
K = 8
NX = 8
NOBS = 2048
NCHUNK = 4096


def box_mean(field, split_axis, reach):
    total = field
    for shift in range(1, reach + 1):
        total = total + jnp.roll(field, shift, split_axis) + jnp.roll(field, -shift, split_axis)
    return total / jnp.sqrt(jnp.float32(2 * reach + 1))


def blended(raw, rough_amp, smooth_amp):
    smooth = box_mean(box_mean(raw, -1, 4), -3, 2)
    return rough_amp * raw + smooth_amp * smooth


def draw_ensemble(key, part):
    first = jax.random.fold_in(key, 11)
    second = jax.random.fold_in(key, 12)
    spots = jnp.arange(NX, dtype=jnp.float32) / max(NX - 1, 1)
    growth = (0.7 * 2.0 ** spots)[:, None, None]
    rough_amp = (1.2 - 0.9 * spots)[:, None, None]
    smooth_amp = (0.3 + 3.0 * spots)[:, None, None]
    height = (jnp.arange(NY, dtype=jnp.float32) + 0.5) / NY * 2.0 - 1.0
    profile = 1.5 * (1.0 - height * height)
    base = jax.random.normal(first, (3, NX, NY, NZ), jnp.float32)
    noise = jax.random.normal(second, (K, 3, NX, NY, NZ), jnp.float32)
    streamwise = (jnp.arange(3) == 0).astype(jnp.float32)[:, None, None, None]
    base = growth * blended(base, rough_amp, smooth_amp) + streamwise * profile[None, None, :, None]
    noise = growth * blended(noise, rough_amp, smooth_amp)
    member_states = base[None] + 0.5 * noise
    return member_states.astype(jnp.float32)


def touch_ends(drawn, own_key, smallest, high):
    longest = drawn.shape.index(max(drawn.shape))
    spots = []
    for shift in (0, 1):
        where = [jax.random.randint(jax.random.fold_in(own_key, axis), (), 0, length) for axis, length in enumerate(drawn.shape)]
        where[longest] = (where[longest] + shift) % drawn.shape[longest]
        spots.append(tuple(where))
    return drawn.at[spots[0]].set(smallest).at[spots[1]].set(high)


def scatter_about(rng, extent, width, most, kind=jnp.bfloat16):
    drawn = width * jax.random.normal(rng, extent, jnp.float32)
    return jnp.clip(drawn, min=-most, max=most).astype(kind)


def setup_inputs(seed: int = 0) -> dict:
    arg_keys = jax.random.split(jax.random.key(seed), 8)
    ensemble = draw_ensemble(jax.random.fold_in(arg_keys[7], 71), 0)
    obs_cell = touch_ends(jax.random.randint(arg_keys[1], (NOBS,), 0, CX * NY * NZ), jax.random.fold_in(arg_keys[1], 1), 0, (CX * NY * NZ) - 1).astype(jnp.int32)
    obs_comp = touch_ends(jax.random.randint(arg_keys[2], (NOBS,), 0, 3), jax.random.fold_in(arg_keys[2], 1), 0, 2).astype(jnp.int32)
    obs_value = scatter_about(arg_keys[3], (NOBS,), 1.0, 6.0, jnp.float32)
    obs_precision = jnp.clip(jnp.exp(jax.random.uniform(arg_keys[4], (NOBS,), jnp.float32, math.log(0.3), math.log(5.0))), 0.3, 5.0)
    loc_obs = touch_ends(jax.random.randint(arg_keys[5], (NCHUNK, LOC), 0, NOBS), jax.random.fold_in(arg_keys[5], 1), 0, NOBS - 1).astype(jnp.int32)
    loc_level = touch_ends(jax.random.randint(arg_keys[6], (NCHUNK, LOC), 1, LEVELS + 1), jax.random.fold_in(arg_keys[6], 1), 1, LEVELS).astype(jnp.int32)
    return {"ensemble": ensemble, "obs_cell": obs_cell, "obs_comp": obs_comp, "obs_value": obs_value, "obs_precision": obs_precision, "loc_obs": loc_obs, "loc_level": loc_level}


PAIRS = ((0, 0), (1, 1), (2, 2), (0, 1), (0, 2), (1, 2))
HIGH = lax.Precision.HIGHEST

def pair_index(first, second):
    for place, pair in enumerate(PAIRS):
        if pair == (first, second) or pair == (second, first):
            return place
    return 0

def pair_weights():
    return jnp.array([1.0, 1.0, 1.0, 2.0, 2.0, 2.0], jnp.float32)[:, None, None, None]

def along_x(field):
    return 0.5 * (field[:, 2:] - field[:, :-2])

def along_y(field):
    rim_extended = jnp.pad(field, ((0, 0), (0, 0), (1, 1), (0, 0)))
    return 0.5 * (rim_extended[:, :, 2:] - rim_extended[:, :, :-2])

def along_z(field):
    return 0.5 * (jnp.roll(field, -1, 3) - jnp.roll(field, 1, 3))

def inner(field):
    return field[:, 1:-1]

def test_filter(field):
    smooth = 0.25 * (field[:, :-2] + 2.0 * field[:, 1:-1] + field[:, 2:])
    return 0.25 * (jnp.roll(smooth, 1, 3) + 2.0 * smooth + jnp.roll(smooth, -1, 3))

def strain(velocity):
    grads = (along_x(velocity), inner(along_y(velocity)), inner(along_z(velocity)))
    return jnp.stack([0.5 * (grads[b][a] + grads[a][b]) for a, b in PAIRS])

def magnitude(rate):
    return jnp.sqrt(2.0 * lax.optimization_barrier(jnp.sum(pair_weights() * rate * rate, 0)))

def eddy_substep(rim_extended, plane_sum, count):
    centre = inner(rim_extended)
    rate = strain(rim_extended)
    size = magnitude(rate)
    smooth = test_filter(rim_extended)
    rate_hat = strain(smooth)
    size_hat = magnitude(rate_hat)
    middle = inner(smooth)
    products = jnp.stack([centre[a] * centre[b] for a, b in PAIRS])
    leonard = test_filter(products) - jnp.stack([middle[a] * middle[b] for a, b in PAIRS])
    model = 2.0 * (test_filter(size[None] * rate) - 4.0 * size_hat[None] * rate_hat)
    weights = pair_weights()
    numer = lax.optimization_barrier(jnp.sum(weights * leonard * model, axis=(0, 1, 3)))
    denom = lax.optimization_barrier(jnp.sum(weights * model * model, axis=(0, 1, 3)))
    numer, denom = plane_sum(numer, denom)
    coeff = numer / count / (denom / count + 1e-06)
    stress = 2.0 * coeff[None, None, :, None] * size[None] * rate
    tendency = []
    for a in range(3):
        term = along_x(stress[pair_index(a, 0)][None])[0]
        term = term + inner(along_y(stress[pair_index(a, 1)][None]))[0]
        term = term + inner(along_z(stress[pair_index(a, 2)][None]))[0]
        tendency.append(term)
    return rim_extended[:, 2:-2] + 0.25 * jnp.stack(tendency)

def bmm(left, right):
    return jnp.einsum('mkc,knc->mnc', left, right, precision=HIGH)

def analyse(block, index, level, anomaly, innov, precision):
    member_states = block.shape[0]
    groups, cols_z = (block.shape[2], block.shape[4])
    cols = index.T
    local = jnp.take(anomaly, cols, axis=1)
    weight = level.T.astype(jnp.float32) / LEVELS * jnp.take(precision, cols)
    scaled = local * weight[None]
    eye = jnp.eye(member_states, dtype=jnp.float32)[:, :, None]
    matrix = jnp.einsum('mjc,njc->mnc', scaled, local, precision=HIGH) + (member_states - 1) / 1.1 * eye
    scale = jnp.sqrt(lax.optimization_barrier(jnp.sum(matrix * matrix, axis=(0, 1))))
    root = matrix / scale
    inverse = jnp.broadcast_to(eye, matrix.shape)
    for sweep in range(NS_ITERS):
        factor = 0.5 * (3.0 * eye - bmm(inverse, root))
        root = bmm(root, factor)
        inverse = bmm(factor, inverse)
    cover = bmm(inverse, inverse) / scale
    drive = jnp.einsum('mjc,jc->mc', scaled, jnp.take(innov, cols), precision=HIGH)
    offset = jnp.einsum('mnc,nc->mc', cover, drive, precision=HIGH)
    transform = jnp.sqrt(member_states - 1.0) * inverse / jnp.sqrt(scale) + offset[:, None, :]
    transform = transform.reshape(member_states, member_states, groups, cols_z // 4)
    transform = jnp.repeat(transform, 4, axis=3)
    centre = lax.optimization_barrier(jnp.mean(block, axis=0))
    spread = block - centre
    moved = jnp.einsum('mqgyz,mkgz->kqgyz', spread, transform, precision=HIGH)
    return centre + moved

def reference(ensemble, obs_cell, obs_comp, obs_value, obs_precision, loc_obs, loc_level):
    member_states = ensemble.shape[0]

    def step_forward(field):
        rim_extended = jnp.concatenate([field[:, -2:], field, field[:, :2]], axis=1)
        return eddy_substep(rim_extended, lambda a, b: (a, b), NX * NZ)
    prior_state = lax.map(step_forward, ensemble)
    grid_cells = NX * NY * NZ
    slab = (jnp.arange(NOBS, dtype=jnp.int32) // NOB_DEV).astype(jnp.int32)
    slab_position = obs_comp * grid_cells + slab * (CX * NY * NZ) + obs_cell
    observed_values = jnp.take(prior_state.reshape(member_states, 3 * grid_cells), slab_position, axis=1)
    mean = lax.optimization_barrier(jnp.mean(observed_values, axis=0))
    anomaly = observed_values - mean[None]
    innov = obs_value - mean
    row_total = NX * NY // 3
    vertical_blocks = NZ // 4
    member_group = 8 if row_total % 8 == 0 else 1
    reshaped_field = prior_state.reshape(member_states, 3, row_total // member_group, member_group, 3, NZ)
    reshaped_field = jnp.transpose(reshaped_field, (2, 0, 1, 3, 4, 5))
    index = loc_obs.reshape(row_total // member_group, member_group * vertical_blocks, LOC)
    level = loc_level.reshape(row_total // member_group, member_group * vertical_blocks, LOC)

    def one(items):
        return analyse(items[0], items[1], items[2], anomaly, innov, obs_precision)
    result = lax.map(one, (reshaped_field, index, level))
    result = jnp.transpose(result, (1, 2, 0, 3, 4, 5))
    return result.reshape(member_states, 3, NX, NY, NZ)
```

```python
import functools

import jax
import jax.numpy as jnp
from jax import lax
from jax.experimental import pallas as pl
from jax.experimental.pallas import tpu as pltpu

NS_ITERS = 8
LEVELS = 8
CHUNK_Y = 3
CHUNK_Z = 4
GROUP = 16
PAIRS = ((0, 0), (1, 1), (2, 2), (0, 1), (0, 2), (1, 2))
WEIGHTS = (1.0, 1.0, 1.0, 2.0, 2.0, 2.0)
PLACE = {}
for _i, (_a, _b) in enumerate(PAIRS):
    PLACE[_a, _b] = PLACE[_b, _a] = _i
MESH = pl.DeviceIdType.MESH
F32 = jnp.float32
BF16 = jnp.bfloat16
NT = (((1,), (1,)), ((), ()))
TN = (((0,), (0,)), ((), ()))


def split3(x):
    hi = x.astype(BF16)
    rest = x - hi.astype(F32)
    mid = rest.astype(BF16)
    low = (rest - mid.astype(F32)).astype(BF16)
    return hi, mid, low


def dz(f):
    return pltpu.roll(f, f.shape[1] - 1, 1) - pltpu.roll(f, 1, 1)


def dy(f):
    n = f.shape[0]
    row = lax.broadcasted_iota(jnp.int32, f.shape, 0)
    after = jnp.where(row == n - 1, 0.0, pltpu.roll(f, n - 1, 0))
    before = jnp.where(row == 0, 0.0, pltpu.roll(f, 1, 0))
    return after - before


def filt(a, b, c):
    t = a + 2.0 * b + c
    return 0.0625 * (pltpu.roll(t, 1, 1) + 2.0 * t + pltpu.roll(t, t.shape[1] - 1, 1))


def strain(below, here, above):
    gx = [above[a] - below[a] for a in range(3)]
    gy = [dy(here[a]) for a in range(3)]
    gz = [dz(here[a]) for a in range(3)]
    rate = [
        0.5 * gx[0],
        0.5 * gy[1],
        0.5 * gz[2],
        0.25 * (gy[0] + gx[1]),
        0.25 * (gz[0] + gx[2]),
        0.25 * (gz[1] + gy[2]),
    ]
    diag = rate[0] * rate[0] + rate[1] * rate[1] + rate[2] * rate[2]
    off = rate[3] * rate[3] + rate[4] * rate[4] + rate[5] * rate[5]
    return rate, jnp.sqrt(2.0 * (diag + 2.0 * off))


def products(left, right, k):
    return [sum(left[m][j : j + 1, :] * right[j] for j in range(k)) for m in range(k)]


def transform_small(amat, drive, k, cols):
    row = lax.broadcasted_iota(jnp.int32, (k, cols), 0)
    eye = [jnp.where(row == m, 1.0, 0.0).astype(F32) for m in range(k)]
    matrix = [amat[m * k : (m + 1) * k, :] + ((k - 1) / 1.1) * eye[m] for m in range(k)]
    scale = jnp.sqrt(jnp.sum(sum(v * v for v in matrix), axis=0, keepdims=True))
    inv_scale = 1.0 / scale
    root = [v * inv_scale for v in matrix]
    inverse = eye
    for sweep in range(NS_ITERS):
        zy = products(inverse, root, k) if sweep else root
        factor = [1.5 * eye[m] - 0.5 * zy[m] for m in range(k)]
        if sweep < NS_ITERS - 1:
            root = products(root, factor, k)
        inverse = products(factor, inverse, k) if sweep else factor
    cover = products(inverse, inverse, k)
    gain = jnp.sqrt(k - 1.0) / jnp.sqrt(scale)
    out = []
    for m in range(k):
        wbar = jnp.sum(cover[m] * drive, axis=0, keepdims=True) * inv_scale
        out.append(gain * inverse[m] + wbar)
    return out


def transform_large(amat, drive, k, cols, zr, yr, tr, ur):
    def each(fn):
        lax.fori_loop(0, k, lambda m, c: (fn(m), c)[1], 0)

    row = lax.broadcasted_iota(jnp.int32, (k, cols), 0)

    def eye(m):
        return jnp.where(row == m, 1.0, 0.0).astype(F32)

    def product(left, right, out, post):
        def one(m):
            def step(j, acc):
                return acc + left[m, pl.ds(j, 1), :] * right[j]

            out[m] = post(m, lax.fori_loop(0, k, step, jnp.zeros((k, cols), F32)))

        each(one)

    for m in range(k):
        yr[m] = amat[m * k : (m + 1) * k, :] + ((k - 1) / 1.1) * eye(m)
        zr[m] = eye(m)
    total = lax.fori_loop(0, k, lambda m, a: a + yr[m] * yr[m], jnp.zeros((k, cols), F32))
    scale = jnp.sqrt(jnp.sum(total, axis=0, keepdims=True))

    def shrink(m):
        yr[m] = yr[m] / scale

    each(shrink)

    def same(m, v):
        return v

    def copy(src, dst):
        def one(m):
            dst[m] = src[m]

        each(one)

    def sweep(i, c):
        product(zr, yr, tr, lambda m, v: 1.5 * eye(m) - 0.5 * v)
        product(yr, tr, ur, same)
        copy(ur, yr)
        product(tr, zr, ur, same)
        copy(ur, zr)
        return c

    lax.fori_loop(0, NS_ITERS, sweep, 0)
    product(zr, zr, ur, same)
    gain = jnp.sqrt(k - 1.0) / jnp.sqrt(scale)
    return [
        gain * zr[m] + jnp.sum(ur[m] * drive, axis=0, keepdims=True) / scale for m in range(k)
    ]


def kernel(
    dims,
    ens_hbm, cell_hbm, comp_hbm, value_hbm, precision_hbm, loc_hbm, level_hbm, out,
    ens, cell, comp, value, precision, loc, level, load_sem,
    halo, strided, smooth, fore, sums, outbound, block, obs, hx, result, back,
    hist, part_hi, part_lo, pick, gmat, zr, yr, tr, ur,
    halo_send, halo_recv, sum_send, sum_recv, obs_send, obs_recv,
    hx_send, hx_recv, fwd_send, fwd_recv, ret_send, ret_recv,
):
    K, S, CX, NY, NZ, C, NOBS, RR, RP, RB = dims
    me = lax.axis_index("member")
    sl = lax.axis_index("space")
    nob = NOBS // S
    NB = nob // 128
    NH = NOBS // 128

    def member(d):
        return lax.rem(me + d, K)

    def space(d):
        return lax.rem(sl + d, S)

    barrier = pltpu.get_barrier_semaphore()
    partners = [(me, space(b)) for b in range(1, S)] + [(member(a), sl) for a in range(1, K)]
    for to in partners:
        pl.semaphore_signal(barrier, inc=1, device_id=to, device_id_type=MESH)
    loads = [
        pltpu.make_async_copy(src, dst, load_sem.at[i])
        for i, (src, dst) in enumerate(
            ((loc_hbm, loc), (level_hbm, level), (cell_hbm, cell), (comp_hbm, comp),
             (value_hbm, value), (precision_hbm, precision), (ens_hbm, ens))
        )
    ]
    for c in loads:
        c.start()
    pl.semaphore_wait(barrier, len(partners))

    def copy(src, dst, send, recv, to):
        c = pltpu.make_async_remote_copy(
            src_ref=src, dst_ref=dst, send_sem=send, recv_sem=recv, device_id=to, device_id_type=MESH
        )
        c.start()
        return c

    halos = [
        copy(ens_hbm.at[0], halo.at[0], halo_send.at[0], halo_recv.at[0], (me, space(1))),
        copy(ens_hbm.at[0], halo.at[1], halo_send.at[1], halo_recv.at[1], (me, space(S - 1))),
    ]

    for c in loads:
        c.wait()
    iota_hi = lax.broadcasted_iota(jnp.int32, (NH, 128), 0)
    iota_lo = lax.broadcasted_iota(jnp.int32, (128, 128), 0)

    def group(g, carry):
        base = pl.multiple_of(g * GROUP, GROUP)
        index = loc[pl.ds(base, GROUP), :]
        weight = level[pl.ds(base, GROUP), :].astype(F32)
        top = lax.shift_right_logical(index, 7)
        low = jnp.bitwise_and(index, 127)
        for j in range(GROUP):
            a = jnp.where(iota_hi == top[j : j + 1, :], weight[j : j + 1, :], 0.0).astype(BF16)
            b = jnp.where(iota_lo == low[j : j + 1, :], 1.0, 0.0).astype(BF16)
            hist[j * NH : (j + 1) * NH, :] = lax.dot_general(a, b, NT, preferred_element_type=F32)
        for h in range(NH):
            v = hist[pl.ds(h, GROUP, stride=NH), :]
            big = v.astype(BF16)
            part_hi[pl.ds(base, GROUP), h * 128 : (h + 1) * 128] = big
            part_lo[pl.ds(base, GROUP), h * 128 : (h + 1) * 128] = (v - big.astype(F32)).astype(BF16)
        return carry

    lax.fori_loop(0, C // GROUP, group, 0)

    cells = cell[...]
    rows = comp[...] * (CX * NY) + cells // NZ
    lanes = lax.rem(cells, NZ)
    iota_row = lax.broadcasted_iota(jnp.int32, (3 * CX * NY, nob), 0)
    pick[...] = jnp.where(iota_row == rows, 1.0, 0.0).astype(BF16)

    for c in halos:
        c.wait_recv()

    def u(a, i):
        if i < 2:
            return halo[0, a, CX - 2 + i]
        if i < 2 + CX:
            return ens[0, a, i - 2]
        return halo[1, a, i - 2 - CX]

    mids = range(1, CX + 3)
    for i in mids:
        rate, size = strain(*[[u(a, i + s) for a in range(3)] for s in (-1, 0, 1)])
        for p in range(6):
            strided[p, i - 1] = size * rate[p]
        for a in range(3):
            smooth[a, i - 1] = filt(u(a, i - 1), u(a, i), u(a, i + 1))
    numer = jnp.zeros((NY, NZ), F32)
    denom = jnp.zeros((NY, NZ), F32)
    for i in range(2, CX + 2):
        rate, size = strain(*[[smooth[a, i - 1 + s] for a in range(3)] for s in (-1, 0, 1)])
        for p, (a, b) in enumerate(PAIRS):
            prod = filt(*[u(a, i + s) * u(b, i + s) for s in (-1, 0, 1)])
            leonard = prod - smooth[a, i - 1] * smooth[b, i - 1]
            model = 2.0 * (
                filt(strided[p, i - 2], strided[p, i - 1], strided[p, i]) - 4.0 * size * rate[p]
            )
            numer = numer + WEIGHTS[p] * (leonard * model)
            denom = denom + WEIGHTS[p] * (model * model)
    tiles = NY // 8
    lane = lax.broadcasted_iota(jnp.int32, (8, 128), 1)
    packed = jnp.zeros((8, 128), F32)
    for j in range(tiles):
        at = slice(j * 8, j * 8 + 8)
        packed = jnp.where(lane == j, jnp.sum(numer[at], axis=1, keepdims=True), packed)
        packed = jnp.where(lane == tiles + j, jnp.sum(denom[at], axis=1, keepdims=True), packed)
    sums[sl] = packed
    totals = [
        copy(sums.at[sl], sums.at[sl], sum_send.at[d - 1], sum_recv.at[d - 1], (me, space(d)))
        for d in range(1, S)
    ]
    for c in totals:
        c.wait_recv()
    both = sums[0]
    for s in range(1, S):
        both = both + sums[s]
    count = float(CX * S * NZ)
    below = pltpu.roll(both, 128 - tiles, 1)
    ratio = (both / count) / (below / count + 1e-06)
    coeff = jnp.concatenate(
        [jnp.broadcast_to(ratio[:, j : j + 1], (8, NZ)) for j in range(tiles)], axis=0
    )

    per_layer = NY // RR
    for x in range(CX):
        i = x + 2
        for a in range(3):
            px, py, pz = (PLACE[a, b] for b in range(3))
            flat = strided[px, i] - strided[px, i - 2] + dz(strided[pz, i - 1])
            term = coeff * flat + dy(coeff * strided[py, i - 1])
            f = ens[0, a, x] + 0.25 * term
            fore[(a * CX + x) * NY : (a * CX + x + 1) * NY, :] = f
            for t in range(per_layer):
                p = x * per_layer + t
                outbound[p, a * RR : (a + 1) * RR, :] = f[t * RR : (t + 1) * RR, :]
    parts = split3(fore[...])
    found = sum(lax.dot_general(v, pick[...], TN, preferred_element_type=F32) for v in parts)
    iota_lane = lax.broadcasted_iota(jnp.int32, (NZ, nob), 0)
    seen = jnp.sum(jnp.where(iota_lane == lanes, found, 0.0), axis=0, keepdims=True)
    stack = [seen[:, b * 128 : (b + 1) * 128] for b in range(NB)]
    if RB > NB:
        stack.append(jnp.zeros((RB - NB, 128), F32))
    mine = pl.ds(pl.multiple_of(sl * RB, 8), RB)
    own = pl.ds(pl.multiple_of(me * (S * RB), 8), S * RB)
    tile = jnp.concatenate(stack, axis=0)
    slabs, spread_obs = [], []
    if K * S <= 64:
        here = pl.ds(pl.multiple_of((me * S + sl) * RB, 8), RB)
        obs[0:RB, :] = tile
        for dm in range(K):
            for ds in range(S):
                if dm or ds:
                    at = dm * S + ds
                    spread_obs.append(
                        copy(obs.at[pl.ds(0, RB)], hx.at[here], hx_send.at[at], hx_recv.at[at], (member(dm), space(ds)))
                    )
        hx[here, :] = tile
    else:
        obs[mine, :] = tile
        slabs = [
            copy(obs.at[mine], obs.at[mine], obs_send.at[d - 1], obs_recv.at[d - 1], (me, space(d)))
            for d in range(1, S)
        ]
        for c in slabs:
            c.wait_recv()
        spread_obs = [
            copy(obs, hx.at[own], hx_send.at[d - 1], hx_recv.at[d - 1], (member(d), sl))
            for d in range(1, K)
        ]
        hx[own, :] = obs[...]
    forward = [
        copy(outbound.at[member(d)], block.at[me], fwd_send.at[d - 1], fwd_recv.at[d - 1], (member(d), sl))
        for d in range(1, K)
    ]
    block[me] = outbound[me]

    for c in spread_obs:
        c.wait_recv()

    KK = K * K + K

    def slab_sum(s, acc):
        for b in range(NB):
            h = hx[pl.ds(s * RB + b, K, stride=S * RB), :]
            mean = jnp.sum(h, axis=0, keepdims=True) * (1.0 / K)
            anomaly = h - mean
            at = pl.ds(s * NB + b, 1)
            scaled = anomaly * (precision[at, :] * (1.0 / LEVELS))
            innov = value[at, :] - mean
            rows_g = [anomaly[m : m + 1, :] * scaled for m in range(K)] + [scaled * innov]
            for m, v in enumerate(rows_g):
                for q, w in enumerate(split3(v)):
                    gmat[q, m * K : (m + 1) * K, b * 128 : (b + 1) * 128] = w.astype(F32)
        span = pl.ds(pl.multiple_of(s * nob, 128), nob)
        big, small = part_hi[:, span], part_lo[:, span]
        for q in range(3):
            g = gmat[q].astype(BF16)
            acc = acc + lax.dot_general(g, big, NT, preferred_element_type=F32)
            if q < 2:
                acc = acc + lax.dot_general(g, small, NT, preferred_element_type=F32)
        return acc

    total = jnp.zeros((KK, C), F32)
    if S <= 4:
        for s in range(S):
            total = slab_sum(s, total)
    else:
        total = lax.fori_loop(0, S, slab_sum, total)
    drive = total[K * K :, :]
    if K <= 8:
        weights = transform_small(total, drive, K, C)
    else:
        weights = transform_large(total, drive, K, C, zr, yr, tr, ur)

    blocks_z = NZ // CHUNK_Z
    groups = RR // CHUNK_Y
    ci = lax.broadcasted_iota(jnp.int32, (C, groups * NZ), 0)
    zi = lax.broadcasted_iota(jnp.int32, (C, groups * NZ), 1)
    expand = jnp.where(ci == zi // CHUNK_Z, 1.0, 0.0).astype(BF16)
    wide = sum(
        jnp.dot(v, expand, preferred_element_type=F32)
        for v in split3(jnp.concatenate(weights, axis=0))
    )
    for c in forward:
        c.wait_recv()
    states = [block[m] for m in range(K)]
    centre = sum(states) * (1.0 / K)
    spread = [v - centre for v in states]
    for a in range(3):
        for r in range(RR):
            row = a * RR + r
            z0 = (r // CHUNK_Y) * NZ
            acc = jnp.broadcast_to(centre[row : row + 1, :], (K, NZ))
            for m in range(K):
                acc = acc + spread[m][row : row + 1, :] * wide[m * K : (m + 1) * K, z0 : z0 + NZ]
            result[pl.ds(row, K, stride=RP), :] = acc

    def of(k):
        return pl.ds(pl.multiple_of(k * RP, 8), RP)

    returned = [
        copy(result.at[of(member(d))], back.at[me], ret_send.at[d - 1], ret_recv.at[d - 1], (member(d), sl))
        for d in range(1, K)
    ]
    back[me] = result[of(me), :]
    for c in returned:
        c.wait_recv()
    for p in range(K):
        x, y0 = p // per_layer, (p % per_layer) * RR
        for a in range(3):
            out[0, a, x, y0 : y0 + RR, :] = back[p, a * RR : (a + 1) * RR, :]
    for c in halos + totals + slabs + spread_obs + forward + returned:
        c.wait_send()


def solution(mesh):
    K, S = mesh.shape["member"], mesh.shape["space"]

    def shards(ensemble, obs_cell, obs_comp, obs_value, obs_precision, loc_obs, loc_level):
        CX, NY, NZ = ensemble.shape[2:]
        C = loc_obs.shape[0]
        NOBS = obs_value.shape[0]
        nob = obs_cell.shape[0]
        NH = NOBS // 128
        RR = CX * NY // K
        RP = -(-3 * RR // 8) * 8
        RB = -(-(nob // 128) // 8) * 8
        KK = K * K + K
        dims = (K, S, CX, NY, NZ, C, NOBS, RR, RP, RB)
        large = (K, K, C) if K > 8 else (1, 8, 128)
        dma = pltpu.SemaphoreType.DMA
        hx_copies = K * S if K * S <= 64 else K - 1
        vmem = pl.BlockSpec(memory_space=pltpu.VMEM)
        return pl.pallas_call(
            functools.partial(kernel, dims),
            out_shape=pltpu.VMEM(ensemble.shape, F32),
            in_specs=[pl.BlockSpec(memory_space=pl.ANY)] * 7,
            out_specs=vmem,
            scratch_shapes=[
                pltpu.VMEM(ensemble.shape, F32),
                pltpu.VMEM((1, nob), jnp.int32),
                pltpu.VMEM((1, nob), jnp.int32),
                pltpu.VMEM((NH, 128), F32),
                pltpu.VMEM((NH, 128), F32),
                pltpu.VMEM(loc_obs.shape, jnp.int32),
                pltpu.VMEM(loc_obs.shape, jnp.int32),
                dma((7,)),
                pltpu.VMEM((2, 3, CX, NY, NZ), F32),
                pltpu.VMEM((6, CX + 2, NY, NZ), F32),
                pltpu.VMEM((3, CX + 2, NY, NZ), F32),
                pltpu.VMEM((3 * CX * NY, NZ), F32),
                pltpu.VMEM((S, 8, 128), F32),
                pltpu.VMEM((K, RP, NZ), F32),
                pltpu.VMEM((K, RP, NZ), F32),
                pltpu.VMEM((S * RB, 128), F32),
                pltpu.VMEM((K * S * RB, 128), F32),
                pltpu.VMEM((K * RP, NZ), F32),
                pltpu.VMEM((K, RP, NZ), F32),
                pltpu.VMEM((GROUP * NH, 128), F32),
                pltpu.VMEM((C, NOBS), BF16),
                pltpu.VMEM((C, NOBS), BF16),
                pltpu.VMEM((3 * CX * NY, nob), BF16),
                pltpu.VMEM((3, KK, nob), F32),
                pltpu.VMEM(large, F32),
                pltpu.VMEM(large, F32),
                pltpu.VMEM(large, F32),
                pltpu.VMEM(large, F32),
                dma((2,)), dma((2,)),
                dma((S - 1,)), dma((S - 1,)),
                dma((S - 1,)), dma((S - 1,)),
                dma((hx_copies,)), dma((hx_copies,)),
                dma((K - 1,)), dma((K - 1,)),
                dma((K - 1,)), dma((K - 1,)),
            ],
            compiler_params=pltpu.CompilerParams(
                collective_id=0, has_side_effects=True, vmem_limit_bytes=60000 * 1024
            ),
            name="analysis_step",
        )(
            ensemble,
            obs_cell.reshape(1, nob),
            obs_comp.reshape(1, nob),
            obs_value.reshape(NH, 128),
            obs_precision.reshape(NH, 128),
            loc_obs,
            loc_level,
        )

    from jax.sharding import PartitionSpec as P

    field = P("member", None, "space", None, None)
    local = P(("space", "member"), None)
    return jax.shard_map(
        shards,
        mesh=mesh,
        in_specs=(field, P("space"), P("space"), P(), P(), local, local),
        out_specs=field,
        check_vma=False,
    )
```

```python
import functools

import jax
import jax.numpy as jnp
from jax import lax
from jax.experimental import pallas as pl
from jax.experimental.pallas import tpu as pltpu

NS_ITERS = 8
LEVELS = 8
CHUNK_Y = 3
CHUNK_Z = 4
GROUP = 16
PAIRS = ((0, 0), (1, 1), (2, 2), (0, 1), (0, 2), (1, 2))
WEIGHTS = (1.0, 1.0, 1.0, 2.0, 2.0, 2.0)
PLACE = {}
for _i, (_a, _b) in enumerate(PAIRS):
    PLACE[_a, _b] = PLACE[_b, _a] = _i
MESH = pl.DeviceIdType.MESH
F32 = jnp.float32
BF16 = jnp.bfloat16
NT = (((1,), (1,)), ((), ()))
TN = (((0,), (0,)), ((), ()))


def split2(x):
    hi = x.astype(BF16)
    return hi, (x - hi.astype(F32)).astype(BF16)


def split3(x):
    hi = x.astype(BF16)
    rest = x - hi.astype(F32)
    mid = rest.astype(BF16)
    low = (rest - mid.astype(F32)).astype(BF16)
    return hi, mid, low


def drain(ref, sem):
    pltpu.make_async_copy(ref, ref, sem).wait()


def gather_lanes(table, index):
    return jnp.take_along_axis(table, index, axis=1)


def dz(f):
    return pltpu.roll(f, f.shape[1] - 1, 1) - pltpu.roll(f, 1, 1)


def dy(f):
    n = f.shape[0]
    row = lax.broadcasted_iota(jnp.int32, f.shape, 0)
    after = jnp.where(row == n - 1, 0.0, pltpu.roll(f, n - 1, 0))
    before = jnp.where(row == 0, 0.0, pltpu.roll(f, 1, 0))
    return after - before


def filt(a, b, c):
    t = a + 2.0 * b + c
    return 0.0625 * (pltpu.roll(t, 1, 1) + 2.0 * t + pltpu.roll(t, t.shape[1] - 1, 1))


def strain(below, here, above):
    gx = [above[a] - below[a] for a in range(3)]
    gy = [dy(here[a]) for a in range(3)]
    gz = [dz(here[a]) for a in range(3)]
    rate = [
        0.5 * gx[0],
        0.5 * gy[1],
        0.5 * gz[2],
        0.25 * (gy[0] + gx[1]),
        0.25 * (gz[0] + gx[2]),
        0.25 * (gz[1] + gy[2]),
    ]
    diag = rate[0] * rate[0] + rate[1] * rate[1] + rate[2] * rate[2]
    off = rate[3] * rate[3] + rate[4] * rate[4] + rate[5] * rate[5]
    return rate, jnp.sqrt(2.0 * (diag + 2.0 * off))


def products(left, right, k):
    return [sum(left[m][j : j + 1, :] * right[j] for j in range(k)) for m in range(k)]


def transform_small(amat, drive, k, cols):
    row = lax.broadcasted_iota(jnp.int32, (k, cols), 0)
    eye = [jnp.where(row == m, 1.0, 0.0).astype(F32) for m in range(k)]
    matrix = [amat[m * k : (m + 1) * k, :] + ((k - 1) / 1.1) * eye[m] for m in range(k)]
    scale = jnp.sqrt(jnp.sum(sum(v * v for v in matrix), axis=0, keepdims=True))
    inv_scale = 1.0 / scale
    root = [v * inv_scale for v in matrix]
    inverse = eye
    for sweep in range(NS_ITERS):
        zy = products(inverse, root, k) if sweep else root
        factor = [1.5 * eye[m] - 0.5 * zy[m] for m in range(k)]
        if sweep < NS_ITERS - 1:
            root = products(root, factor, k)
        inverse = products(factor, inverse, k) if sweep else factor
    cover = products(inverse, inverse, k)
    gain = jnp.sqrt(k - 1.0) / jnp.sqrt(scale)
    out = []
    for m in range(k):
        wbar = jnp.sum(cover[m] * drive, axis=0, keepdims=True) * inv_scale
        out.append(gain * inverse[m] + wbar)
    return out


def transform_large(amat, drive, k, cols, zr, yr, tr, ur):
    def each(fn):
        lax.fori_loop(0, k, lambda m, c: (fn(m), c)[1], 0)

    row = lax.broadcasted_iota(jnp.int32, (k, cols), 0)

    def eye(m):
        return jnp.where(row == m, 1.0, 0.0).astype(F32)

    def product(left, right, out, post):
        def one(m):
            def step(j, acc):
                return acc + left[m, pl.ds(j, 1), :] * right[j]

            out[m] = post(m, lax.fori_loop(0, k, step, jnp.zeros((k, cols), F32)))

        each(one)

    for m in range(k):
        yr[m] = amat[m * k : (m + 1) * k, :] + ((k - 1) / 1.1) * eye(m)
        zr[m] = eye(m)
    total = lax.fori_loop(0, k, lambda m, a: a + yr[m] * yr[m], jnp.zeros((k, cols), F32))
    scale = jnp.sqrt(jnp.sum(total, axis=0, keepdims=True))

    def shrink(m):
        yr[m] = yr[m] / scale

    each(shrink)

    def same(m, v):
        return v

    def copy(src, dst):
        def one(m):
            dst[m] = src[m]

        each(one)

    def sweep(i, c):
        product(zr, yr, tr, lambda m, v: 1.5 * eye(m) - 0.5 * v)
        product(yr, tr, ur, same)
        copy(ur, yr)
        product(tr, zr, ur, same)
        copy(ur, zr)
        return c

    lax.fori_loop(0, NS_ITERS, sweep, 0)
    product(zr, zr, ur, same)
    gain = jnp.sqrt(k - 1.0) / jnp.sqrt(scale)
    return [
        gain * zr[m] + jnp.sum(ur[m] * drive, axis=0, keepdims=True) / scale for m in range(k)
    ]


def kernel(
    dims,
    ens_hbm, cell_hbm, tile_hbm, comp_hbm, value_hbm, precision_hbm, loc_hbm, level_hbm, out,
    ens, cell, cells2, comp, value, precision, local, load_sem,
    halo, strided, smooth, flats, early, places, late, outbound, block, hx, result, back,
    hist, parts, pick, expand, gmat, zr, yr, tr, ur,
    halo_send, halo_recv, early_send, early_recv, place_send, place_recv,
    late_send, late_recv, hx_send, hx_recv, fwd_send, fwd_recv, ret_send, ret_recv,
):
    K, S, CX, NY, NZ, C, NOBS, RR, RP = dims
    me = lax.axis_index("member")
    sl = lax.axis_index("space")
    nob = NOBS // S
    NB = nob // 128
    NH = NOBS // 128
    R = 3 * CX * NY
    T = 2 * NB

    def member(d):
        return lax.rem(me + d, K)

    def space(d):
        return lax.rem(sl + d, S)

    barrier = pltpu.get_barrier_semaphore()
    partners = [(me, space(b)) for b in range(1, S)] + [(member(a), sl) for a in range(1, K)]
    for to in partners:
        pl.semaphore_signal(barrier, inc=1, device_id=to, device_id_type=MESH)
    loads = [
        pltpu.make_async_copy(src, dst, load_sem.at[i])
        for i, (src, dst) in enumerate(
            ((cell_hbm, cell), (tile_hbm, cells2), (comp_hbm, comp), (ens_hbm, ens),
             (loc_hbm, local.at[0]), (level_hbm, local.at[1]), (value_hbm, value), (precision_hbm, precision))
        )
    ]
    for c in loads:
        c.start()
    pl.semaphore_wait(barrier, len(partners))

    def copy(src, dst, send, recv, to):
        pltpu.make_async_remote_copy(
            src_ref=src, dst_ref=dst, send_sem=send, recv_sem=recv, device_id=to, device_id_type=MESH
        ).start()

    copy(ens_hbm.at[0], halo.at[0], halo_send, halo_recv, (me, space(1)))
    copy(ens_hbm.at[0], halo.at[1], halo_send, halo_recv, (me, space(S - 1)))
    for c in loads:
        c.wait()

    row_t = lax.broadcasted_iota(jnp.int32, (T, 128), 0)
    lane_t = lax.broadcasted_iota(jnp.int32, (T, 128), 1)
    cells = cell[...]
    lanes = lax.rem(cells, NZ)
    levels = cells // NZ
    heights = lax.rem(levels, NY)
    rows = comp[...] * (CX * NY) + levels
    iota_lane = lax.broadcasted_iota(jnp.int32, (NZ, nob), 0)
    one_hot = jnp.where(iota_lane == lanes, 1.0, 0.0).astype(BF16)
    pick[0:NZ, :] = one_hot
    pick[NZ:, :] = one_hot
    eighth = lax.broadcasted_iota(jnp.int32, (8, nob), 0)
    here = rows - eighth
    after = jnp.where(heights == NY - 1, -R, rows + 1) - eighth
    before = jnp.where(heights == 0, -R, rows - 1) - eighth

    def of_lanes(field):
        return jnp.dot(
            jnp.concatenate(split2(field), axis=1), pick[...], preferred_element_type=F32
        )

    def of_rows(found, wanted):
        acc = jnp.zeros((8, nob), F32)
        for t in range(R // 8):
            acc = acc + jnp.where(wanted == 8 * t, found[8 * t : 8 * t + 8, :], 0.0)
        seen = jnp.sum(acc, axis=0, keepdims=True)
        return [seen[:, b * 128 : (b + 1) * 128] for b in range(NB)]

    def tile_of(values):
        tile = jnp.zeros((T, 128), F32)
        for r, v in enumerate(values):
            tile = jnp.where(row_t == r, v, tile)
        return tile

    at_cells = lax.rem(cells2[...] // NZ, NY)
    places[sl] = jnp.concatenate([at_cells, at_cells], axis=0)
    fields = jnp.concatenate([ens[0, a, x] for a in range(3) for x in range(CX)], axis=0)
    found = sum(
        jnp.dot(v, pick[0:NZ, :], preferred_element_type=F32) for v in split3(fields)
    )
    seen = of_rows(found, here)
    early[sl] = tile_of(seen + seen)
    for d in range(1, S):
        copy(places.at[sl], places.at[sl], place_send, place_recv, (me, space(d)))
        copy(early.at[sl], early.at[sl], early_send, early_recv, (me, space(d)))

    iota_hi = lax.broadcasted_iota(jnp.int32, (NH, 128), 0)
    iota_lo = lax.broadcasted_iota(jnp.int32, (128, 128), 0)

    def group(g, carry):
        base = pl.multiple_of(g * GROUP, GROUP)
        index = local[0, pl.ds(base, GROUP), :]
        weight = local[1, pl.ds(base, GROUP), :].astype(F32)
        top = lax.shift_right_logical(index, 7)
        low = jnp.bitwise_and(index, 127)
        for j in range(GROUP):
            a = jnp.where(iota_hi == top[j : j + 1, :], weight[j : j + 1, :], 0.0).astype(BF16)
            b = jnp.where(iota_lo == low[j : j + 1, :], 1.0, 0.0).astype(BF16)
            hist[j * NH : (j + 1) * NH, :] = lax.dot_general(a, b, NT, preferred_element_type=F32)
        for h in range(NH):
            big, small = split2(hist[pl.ds(h, GROUP, stride=NH), :])
            parts[pl.ds(base, GROUP), h * 128 : (h + 1) * 128] = big
            parts[pl.ds(C + base, GROUP), h * 128 : (h + 1) * 128] = small
        return carry

    lax.fori_loop(0, C // GROUP, group, 0)

    blocks_z = NZ // CHUNK_Z
    groups = RR // CHUNK_Y
    ci = lax.broadcasted_iota(jnp.int32, (C, groups * NZ), 0)
    zi = lax.broadcasted_iota(jnp.int32, (C, groups * NZ), 1)
    spread_z = jnp.where(ci == zi // CHUNK_Z, 1.0, 0.0).astype(BF16)
    expand[0:C, :] = spread_z
    expand[C:, :] = spread_z

    drain(halo, halo_recv)

    def u(a, i):
        if i < 2:
            return halo[0, a, CX - 2 + i]
        if i < 2 + CX:
            return ens[0, a, i - 2]
        return halo[1, a, i - 2 - CX]

    mids = range(1, CX + 3)
    for i in mids:
        rate, size = strain(*[[u(a, i + s) for a in range(3)] for s in (-1, 0, 1)])
        for p in range(6):
            strided[p, i - 1] = size * rate[p]
    for x in range(CX):
        i = x + 2
        for a in range(3):
            px, pz = PLACE[a, 0], PLACE[a, 2]
            flats[(a * CX + x) * NY : (a * CX + x + 1) * NY, :] = (
                strided[px, i] - strided[px, i - 2] + dz(strided[pz, i - 1])
            )
    along_y = jnp.concatenate(
        [strided[PLACE[a, 1], x + 1] for a in range(3) for x in range(CX)], axis=0
    )
    found = of_lanes(flats[...])
    first = of_rows(found, here)
    found = of_lanes(along_y)
    first = first + of_rows(found, after)
    second = of_rows(found, before)
    for i in mids:
        for a in range(3):
            smooth[a, i - 1] = filt(u(a, i - 1), u(a, i), u(a, i + 1))
    numer = jnp.zeros((NY, NZ), F32)
    denom = jnp.zeros((NY, NZ), F32)
    for i in range(2, CX + 2):
        rate, size = strain(*[[smooth[a, i - 1 + s] for a in range(3)] for s in (-1, 0, 1)])
        for p, (a, b) in enumerate(PAIRS):
            prod = filt(*[u(a, i + s) * u(b, i + s) for s in (-1, 0, 1)])
            leonard = prod - smooth[a, i - 1] * smooth[b, i - 1]
            model = 2.0 * (
                filt(strided[p, i - 2], strided[p, i - 1], strided[p, i]) - 4.0 * size * rate[p]
            )
            numer = numer + WEIGHTS[p] * (leonard * model)
            denom = denom + WEIGHTS[p] * (model * model)
    tiles = NY // 8
    row_8 = lax.broadcasted_iota(jnp.int32, (8, 128), 0)
    lane_8 = lax.broadcasted_iota(jnp.int32, (8, 128), 1)
    planes = []
    for v in (numer, denom):
        packed = jnp.zeros((8, 128), F32)
        for j in range(tiles):
            total = jnp.sum(v[j * 8 : j * 8 + 8], axis=1, keepdims=True)
            packed = jnp.where(lane_8 == j, total, packed)
        packed = gather_lanes(packed, lane_8 // 8)
        packed = jnp.where(lax.rem(lane_8, 8) == row_8, packed, 0.0)
        planes.append(jnp.sum(packed, axis=0, keepdims=True))
    late[sl, 0] = tile_of(first)
    late[sl, 1] = tile_of(second + planes)
    for d in range(1, S):
        copy(late.at[sl], late.at[sl], late_send, late_recv, (me, space(d)))

    drain(early.at[0 : S - 1], early_recv)
    drain(places.at[0 : S - 1], place_recv)
    drain(late.at[0 : S - 1], late_recv)

    count = float(CX * S * NZ)
    above, below = [
        sum(jnp.broadcast_to(late[s, 1, NB + q : NB + q + 1, :], (T, 128)) for s in range(S))
        for q in range(2)
    ]
    ratio = jnp.where(lane_t < NY, (above / count) / (below / count + 1e-06), 0.0)
    quarter = 0.25 * ratio
    values = []
    for s in range(S):
        y = places[s]
        ya = jnp.where(row_t < NB, y, y + 1)
        yb = jnp.maximum(y - 1, 0)
        v = late[s, 0] * gather_lanes(quarter, ya)
        v = v - jnp.where(row_t < NB, late[s, 1] * gather_lanes(quarter, yb), 0.0)
        values.append(v + pltpu.roll(v, NB, 0) + early[s])
    own = pl.ds(pl.multiple_of(me * NH, 8), NH)
    hx[own, :] = jnp.concatenate(
        [jnp.where(row_t < NB, values[s], values[s + 1]) for s in range(0, S, 2)], axis=0
    )
    for d in range(1, K):
        copy(hx.at[own], hx.at[own], hx_send, hx_recv, (member(d), sl))

    coeff = jnp.concatenate(
        [gather_lanes(ratio[0:8], 8 * j + row_8) for j in range(tiles)], axis=0
    )
    per_layer = NY // RR
    for x in range(CX):
        for a in range(3):
            flat = flats[(a * CX + x) * NY : (a * CX + x + 1) * NY, :]
            term = coeff * flat + dy(coeff * strided[PLACE[a, 1], x + 1])
            f = ens[0, a, x] + 0.25 * term
            for t in range(per_layer):
                p = x * per_layer + t
                outbound[p, a * RR : (a + 1) * RR, :] = f[t * RR : (t + 1) * RR, :]
    for d in range(1, K):
        copy(outbound.at[member(d)], block.at[me], fwd_send, fwd_recv, (member(d), sl))
    block[me] = outbound[me]

    drain(hx.at[pl.ds(0, (K - 1) * NH)], hx_recv)

    KK = K * K
    pair = max(1, 16 // K)
    fused = C % 128 == 0

    def slab_sum(s, acc):
        for b in range(NB):
            h = hx[pl.ds(s * NB + b, K, stride=NH), :]
            mean = jnp.sum(h, axis=0, keepdims=True) * (1.0 / K)
            anomaly = h - mean
            at = pl.ds(s * NB + b, 1)
            scaled = anomaly * (precision[at, :] * (1.0 / LEVELS))
            innov = value[at, :] - mean
            span = slice(b * 128, (b + 1) * 128)
            for m in range(0, K, pair):
                v = jnp.concatenate([anomaly[q : q + 1, :] * scaled for q in range(m, m + pair)], axis=0)
                hi, lo = split2(v)
                gmat[m * K : (m + pair) * K, span] = hi
                gmat[KK + m * K : KK + (m + pair) * K, span] = lo
            v = scaled * innov
            hi = v.astype(BF16).astype(F32)
            gmat[2 * KK :, span] = jnp.concatenate([hi, v - hi], axis=0).astype(BF16)
        span = pl.ds(pl.multiple_of(s * nob, 128), nob)
        g = gmat[...]
        if fused:
            return acc + lax.dot_general(g, parts[:, span], NT, preferred_element_type=F32)
        for q in range(2):
            acc = acc + lax.dot_general(
                g, parts[q * C : (q + 1) * C, span], NT, preferred_element_type=F32
            )
        return acc

    total = jnp.zeros((2 * (KK + K), 2 * C if fused else C), F32)
    if S <= 4:
        for s in range(S):
            total = slab_sum(s, total)
    else:
        total = lax.fori_loop(0, S, slab_sum, total)
    if fused:
        total = total[:, :C] + total[:, C:]
    amat = total[:KK] + total[KK : 2 * KK]
    drive = total[2 * KK : 2 * KK + K] + total[2 * KK + K :]
    if K <= 8:
        weights = transform_small(amat, drive, K, C)
    else:
        weights = transform_large(amat, drive, K, C, zr, yr, tr, ur)

    narrow = split2(jnp.concatenate(weights, axis=0))
    if fused:
        wide = jnp.dot(jnp.concatenate(narrow, axis=1), expand[...], preferred_element_type=F32)
    else:
        wide = sum(jnp.dot(v, expand[0:C, :], preferred_element_type=F32) for v in narrow)
    drain(block.at[0 : K - 1], fwd_recv)
    states = [block[m] for m in range(K)]
    centre = sum(states) * (1.0 / K)
    spread = [v - centre for v in states]
    for a in range(3):
        for r in range(RR):
            row = a * RR + r
            z0 = (r // CHUNK_Y) * NZ
            acc = jnp.broadcast_to(centre[row : row + 1, :], (K, NZ))
            for m in range(K):
                acc = acc + spread[m][row : row + 1, :] * wide[m * K : (m + 1) * K, z0 : z0 + NZ]
            result[pl.ds(row, K, stride=RP), :] = acc

    def of(k):
        return pl.ds(pl.multiple_of(k * RP, 8), RP)

    for d in range(1, K):
        copy(result.at[of(member(d))], back.at[me], ret_send, ret_recv, (member(d), sl))
    back[me] = result[of(me), :]
    drain(back.at[0 : K - 1], ret_recv)
    for p in range(K):
        x, y0 = p // per_layer, (p % per_layer) * RR
        for a in range(3):
            out[0, a, x, y0 : y0 + RR, :] = back[p, a * RR : (a + 1) * RR, :]
    drain(halo, halo_send)
    drain(places.at[0 : S - 1], place_send)
    drain(early.at[0 : S - 1], early_send)
    drain(late.at[0 : S - 1], late_send)
    drain(hx.at[pl.ds(0, (K - 1) * NH)], hx_send)
    drain(block.at[0 : K - 1], fwd_send)
    drain(back.at[0 : K - 1], ret_send)


def solution(mesh):
    K, S = mesh.shape["member"], mesh.shape["space"]

    def shards(ensemble, obs_cell, obs_comp, obs_value, obs_precision, loc_obs, loc_level):
        CX, NY, NZ = ensemble.shape[2:]
        C = loc_obs.shape[0]
        NOBS = obs_value.shape[0]
        nob = obs_cell.shape[0]
        NB = nob // 128
        NH = NOBS // 128
        RR = CX * NY // K
        RP = -(-3 * RR // 8) * 8
        KK = K * K + K
        T = 2 * NB
        dims = (K, S, CX, NY, NZ, C, NOBS, RR, RP)
        large = (K, K, C) if K > 8 else (1, 8, 128)
        dma = pltpu.SemaphoreType.DMA
        vmem = pl.BlockSpec(memory_space=pltpu.VMEM)
        return pl.pallas_call(
            functools.partial(kernel, dims),
            out_shape=pltpu.VMEM(ensemble.shape, F32),
            in_specs=[pl.BlockSpec(memory_space=pl.ANY)] * 8,
            out_specs=vmem,
            scratch_shapes=[
                pltpu.VMEM(ensemble.shape, F32),
                pltpu.VMEM((1, nob), jnp.int32),
                pltpu.VMEM((NB, 128), jnp.int32),
                pltpu.VMEM((1, nob), jnp.int32),
                pltpu.VMEM((NH, 128), F32),
                pltpu.VMEM((NH, 128), F32),
                pltpu.VMEM((2, *loc_obs.shape), jnp.int32),
                dma((8,)),
                pltpu.VMEM((2, 3, CX, NY, NZ), F32),
                pltpu.VMEM((6, CX + 2, NY, NZ), F32),
                pltpu.VMEM((3, CX + 2, NY, NZ), F32),
                pltpu.VMEM((3 * CX * NY, NZ), F32),
                pltpu.VMEM((S, T, 128), F32),
                pltpu.VMEM((S, T, 128), jnp.int32),
                pltpu.VMEM((S, 2, T, 128), F32),
                pltpu.VMEM((K, RP, NZ), F32),
                pltpu.VMEM((K, RP, NZ), F32),
                pltpu.VMEM((K * NH, 128), F32),
                pltpu.VMEM((K * RP, NZ), F32),
                pltpu.VMEM((K, RP, NZ), F32),
                pltpu.VMEM((GROUP * NH, 128), F32),
                pltpu.VMEM((2 * C, NOBS), BF16),
                pltpu.VMEM((2 * NZ, nob), BF16),
                pltpu.VMEM((2 * C, RR // CHUNK_Y * NZ), BF16),
                pltpu.VMEM((2 * KK, nob), BF16),
                pltpu.VMEM(large, F32),
                pltpu.VMEM(large, F32),
                pltpu.VMEM(large, F32),
                pltpu.VMEM(large, F32),
            ] + [dma] * 14,
            compiler_params=pltpu.CompilerParams(
                collective_id=0, has_side_effects=True, vmem_limit_bytes=60000 * 1024
            ),
            name="analysis_step",
        )(
            ensemble,
            obs_cell.reshape(1, nob),
            obs_cell.reshape(NB, 128),
            obs_comp.reshape(1, nob),
            obs_value.reshape(NH, 128),
            obs_precision.reshape(NH, 128),
            loc_obs,
            loc_level,
        )

    from jax.sharding import PartitionSpec as P

    field = P("member", None, "space", None, None)
    local = P(("space", "member"), None)
    return jax.shard_map(
        shards,
        mesh=mesh,
        in_specs=(field, P("space"), P("space"), P(), P(), local, local),
        out_specs=field,
        check_vma=False,
    )
```

```python
import functools

import jax
import jax.numpy as jnp
from jax import lax
from jax.experimental import pallas as pl
from jax.experimental.pallas import tpu as pltpu

NS_ITERS = 8
LEVELS = 8
CHUNK_Y = 3
CHUNK_Z = 4
GROUP = 16
PAIRS = ((0, 0), (1, 1), (2, 2), (0, 1), (0, 2), (1, 2))
WEIGHTS = (1.0, 1.0, 1.0, 2.0, 2.0, 2.0)
PLACE = {}
for _i, (_a, _b) in enumerate(PAIRS):
    PLACE[_a, _b] = PLACE[_b, _a] = _i
MESH = pl.DeviceIdType.MESH
F32 = jnp.float32
BF16 = jnp.bfloat16
NT = (((1,), (1,)), ((), ()))
TN = (((0,), (0,)), ((), ()))


def split2(x):
    hi = x.astype(BF16)
    return hi, (x - hi.astype(F32)).astype(BF16)


def split3(x):
    hi = x.astype(BF16)
    rest = x - hi.astype(F32)
    mid = rest.astype(BF16)
    low = (rest - mid.astype(F32)).astype(BF16)
    return hi, mid, low


def drain(ref, sem):
    pltpu.make_async_copy(ref, ref, sem).wait()


def gather_lanes(table, index):
    return jnp.take_along_axis(table, index, axis=1)


def dz(f):
    return pltpu.roll(f, f.shape[1] - 1, 1) - pltpu.roll(f, 1, 1)


def dy(f):
    n = f.shape[0]
    row = lax.broadcasted_iota(jnp.int32, f.shape, 0)
    after = jnp.where(row == n - 1, 0.0, pltpu.roll(f, n - 1, 0))
    before = jnp.where(row == 0, 0.0, pltpu.roll(f, 1, 0))
    return after - before


def filt(a, b, c):
    t = a + 2.0 * b + c
    return 0.0625 * (pltpu.roll(t, 1, 1) + 2.0 * t + pltpu.roll(t, t.shape[1] - 1, 1))


def strain(below, here, above):
    gx = [above[a] - below[a] for a in range(3)]
    gy = [dy(here[a]) for a in range(3)]
    gz = [dz(here[a]) for a in range(3)]
    rate = [
        0.5 * gx[0],
        0.5 * gy[1],
        0.5 * gz[2],
        0.25 * (gy[0] + gx[1]),
        0.25 * (gz[0] + gx[2]),
        0.25 * (gz[1] + gy[2]),
    ]
    diag = rate[0] * rate[0] + rate[1] * rate[1] + rate[2] * rate[2]
    off = rate[3] * rate[3] + rate[4] * rate[4] + rate[5] * rate[5]
    return rate, jnp.sqrt(2.0 * (diag + 2.0 * off))


def products(left, right, k):
    return [sum(left[m][j : j + 1, :] * right[j] for j in range(k)) for m in range(k)]


def transform_small(amat, drive, k, cols):
    row = lax.broadcasted_iota(jnp.int32, (k, cols), 0)
    eye = [jnp.where(row == m, 1.0, 0.0).astype(F32) for m in range(k)]
    matrix = [amat[m * k : (m + 1) * k, :] + ((k - 1) / 1.1) * eye[m] for m in range(k)]
    scale = jnp.sqrt(jnp.sum(sum(v * v for v in matrix), axis=0, keepdims=True))
    inv_scale = 1.0 / scale
    root = [v * inv_scale for v in matrix]
    inverse = eye
    for sweep in range(NS_ITERS):
        zy = products(inverse, root, k) if sweep else root
        factor = [1.5 * eye[m] - 0.5 * zy[m] for m in range(k)]
        if sweep < NS_ITERS - 1:
            root = products(root, factor, k)
        inverse = products(factor, inverse, k) if sweep else factor
    cover = products(inverse, inverse, k)
    gain = jnp.sqrt(k - 1.0) / jnp.sqrt(scale)
    out = []
    for m in range(k):
        wbar = jnp.sum(cover[m] * drive, axis=0, keepdims=True) * inv_scale
        out.append(gain * inverse[m] + wbar)
    return out


def transform_large(amat, drive, k, cols, zr, yr, tr, ur):
    def each(fn):
        lax.fori_loop(0, k, lambda m, c: (fn(m), c)[1], 0)

    row = lax.broadcasted_iota(jnp.int32, (k, cols), 0)

    def eye(m):
        return jnp.where(row == m, 1.0, 0.0).astype(F32)

    def product(left, right, out, post):
        def one(m):
            def step(j, acc):
                return acc + left[m, pl.ds(j, 1), :] * right[j]

            out[m] = post(m, lax.fori_loop(0, k, step, jnp.zeros((k, cols), F32)))

        each(one)

    for m in range(k):
        yr[m] = amat[m * k : (m + 1) * k, :] + ((k - 1) / 1.1) * eye(m)
        zr[m] = eye(m)
    total = lax.fori_loop(0, k, lambda m, a: a + yr[m] * yr[m], jnp.zeros((k, cols), F32))
    scale = jnp.sqrt(jnp.sum(total, axis=0, keepdims=True))

    def shrink(m):
        yr[m] = yr[m] / scale

    each(shrink)

    def same(m, v):
        return v

    def copy(src, dst):
        def one(m):
            dst[m] = src[m]

        each(one)

    def sweep(i, c):
        product(zr, yr, tr, lambda m, v: 1.5 * eye(m) - 0.5 * v)
        product(yr, tr, ur, same)
        copy(ur, yr)
        product(tr, zr, ur, same)
        copy(ur, zr)
        return c

    lax.fori_loop(0, NS_ITERS, sweep, 0)
    product(zr, zr, ur, same)
    gain = jnp.sqrt(k - 1.0) / jnp.sqrt(scale)
    return [
        gain * zr[m] + jnp.sum(ur[m] * drive, axis=0, keepdims=True) / scale for m in range(k)
    ]


def kernel(
    dims,
    ens_hbm, cell_hbm, tile_hbm, comp_hbm, value_hbm, precision_hbm, loc_hbm, level_hbm, out,
    ens, cell, cells2, comp, value, precision, local, load_sem,
    halo, strided, smooth, flats, early, places, late, outbound, block, hx, result, back,
    hist, parts, pick, expand, gmat, zr, yr, tr, ur,
    halo_send, halo_recv, early_send, early_recv, place_send, place_recv,
    late_send, late_recv, hx_send, hx_recv, fwd_send, fwd_recv, ret_send, ret_recv, near_sem, far_sem, wrap_sem, ready_sem,
):
    K, S, CX, NY, NZ, C, NOBS, RR, RP = dims
    me = lax.axis_index("member")
    sl = lax.axis_index("space")
    nob = NOBS // S
    NB = nob // 128
    NH = NOBS // 128
    R = 3 * CX * NY
    T = 2 * NB
    short = S == 4

    def mate(d):
        bit, to = 1, me
        while bit < K:
            if d // bit % 2:
                to = to + bit - 2 * bit * lax.rem(me // bit, 2)
            bit *= 2
        return to

    def space(d):
        return lax.rem(sl + d, S)

    barrier = pltpu.get_barrier_semaphore()
    mates = [(mate(a), sl) for a in range(K - 1, 0, -1)]
    columns = [(me, space(b)) for b in range(1, S)]

    def tell(sem, to):
        pl.semaphore_signal(sem, inc=1, device_id=to, device_id_type=MESH)

    if short:
        root, hub = sl == 0, sl == S - 2

        @pl.when(root)
        def _():
            tell(barrier, (me, space(S - 1)))

        @pl.when(jnp.logical_or(root, hub))
        def _():
            tell(barrier, (me, space(1)))

        @pl.when(sl == 1)
        def _():
            tell(barrier, (me, space(S - 1)))

        @pl.when(hub)
        def _():
            tell(barrier, (me, space(S - 1)))
            for to in mates:
                tell(barrier, to)
    else:
        for to in columns + mates:
            tell(barrier, to)
    loads = [
        pltpu.make_async_copy(src, dst, load_sem.at[i])
        for i, (src, dst) in enumerate(
            ((cell_hbm, cell), (tile_hbm, cells2), (comp_hbm, comp), (ens_hbm, ens),
             (loc_hbm, local.at[0]), (level_hbm, local.at[1]), (value_hbm, value), (precision_hbm, precision))
        )
    ]
    for c in loads:
        c.start()
    if short:

        @pl.when(sl != S - 2)
        def _():
            pl.semaphore_wait(barrier, 2 - jnp.where(root, 1, 0))

        @pl.when(sl == 1)
        def _():
            tell(near_sem, (me, space(1)))

        @pl.when(sl == S - 1)
        def _():
            tell(far_sem, (me, space(S - 1)))
            tell(wrap_sem, (me, space(1)))

        @pl.when(hub)
        def _():
            pl.semaphore_wait(far_sem, 1)
            pl.semaphore_wait(near_sem, 1)
    else:
        pl.semaphore_wait(barrier, S - 1 + len(mates))

    def copy(src, dst, send, recv, to):
        pltpu.make_async_remote_copy(
            src_ref=src, dst_ref=dst, send_sem=send, recv_sem=recv, device_id=to, device_id_type=MESH
        ).start()

    copy(ens_hbm.at[0], halo.at[0], halo_send, halo_recv, (me, space(1)))
    if short:

        @pl.when(root)
        def _():
            pl.semaphore_wait(wrap_sem, 1)

    copy(ens_hbm.at[0], halo.at[1], halo_send, halo_recv, (me, space(S - 1)))
    for c in loads:
        c.wait()

    row_t = lax.broadcasted_iota(jnp.int32, (T, 128), 0)
    lane_t = lax.broadcasted_iota(jnp.int32, (T, 128), 1)
    cells = cell[...]
    lanes = lax.rem(cells, NZ)
    levels = cells // NZ
    heights = lax.rem(levels, NY)
    rows = comp[...] * (CX * NY) + levels
    iota_lane = lax.broadcasted_iota(jnp.int32, (NZ, nob), 0)
    one_hot = jnp.where(iota_lane == lanes, 1.0, 0.0).astype(BF16)
    pick[0:NZ, :] = one_hot
    pick[NZ:, :] = one_hot
    eighth = lax.broadcasted_iota(jnp.int32, (8, nob), 0)
    here = rows - eighth
    after = jnp.where(heights == NY - 1, -R, rows + 1) - eighth
    before = jnp.where(heights == 0, -R, rows - 1) - eighth

    def of_lanes(field):
        return jnp.dot(
            jnp.concatenate(split2(field), axis=1), pick[...], preferred_element_type=F32
        )

    def of_rows(found, wanted):
        acc = jnp.zeros((8, nob), F32)
        for t in range(R // 8):
            acc = acc + jnp.where(wanted == 8 * t, found[8 * t : 8 * t + 8, :], 0.0)
        seen = jnp.sum(acc, axis=0, keepdims=True)
        return [seen[:, b * 128 : (b + 1) * 128] for b in range(NB)]

    def tile_of(values):
        tile = jnp.zeros((T, 128), F32)
        for r, v in enumerate(values):
            tile = jnp.where(row_t == r, v, tile)
        return tile

    at_cells = lax.rem(cells2[...] // NZ, NY)
    places[sl] = jnp.concatenate([at_cells, at_cells], axis=0)
    fields = jnp.concatenate([ens[0, a, x] for a in range(3) for x in range(CX)], axis=0)
    found = sum(
        jnp.dot(v, pick[0:NZ, :], preferred_element_type=F32) for v in split3(fields)
    )
    seen = of_rows(found, here)
    early[sl] = tile_of(seen + seen)

    iota_hi = lax.broadcasted_iota(jnp.int32, (NH, 128), 0)
    iota_lo = lax.broadcasted_iota(jnp.int32, (128, 128), 0)

    def group(g, carry):
        base = pl.multiple_of(g * GROUP, GROUP)
        index = local[0, pl.ds(base, GROUP), :]
        weight = local[1, pl.ds(base, GROUP), :].astype(F32)
        top = lax.shift_right_logical(index, 7)
        low = jnp.bitwise_and(index, 127)
        for j in range(GROUP):
            a = jnp.where(iota_hi == top[j : j + 1, :], weight[j : j + 1, :], 0.0).astype(BF16)
            b = jnp.where(iota_lo == low[j : j + 1, :], 1.0, 0.0).astype(BF16)
            hist[j * NH : (j + 1) * NH, :] = lax.dot_general(a, b, NT, preferred_element_type=F32)
        for h in range(NH):
            big, small = split2(hist[pl.ds(h, GROUP, stride=NH), :])
            parts[pl.ds(base, GROUP), h * 128 : (h + 1) * 128] = big
            parts[pl.ds(C + base, GROUP), h * 128 : (h + 1) * 128] = small
        return carry

    lax.fori_loop(0, C // GROUP, group, 0)

    blocks_z = NZ // CHUNK_Z
    groups = RR // CHUNK_Y
    ci = lax.broadcasted_iota(jnp.int32, (C, groups * NZ), 0)
    zi = lax.broadcasted_iota(jnp.int32, (C, groups * NZ), 1)
    spread_z = jnp.where(ci == zi // CHUNK_Z, 1.0, 0.0).astype(BF16)
    expand[0:C, :] = spread_z
    expand[C:, :] = spread_z

    if short:

        @pl.when(hub)
        def _():
            pl.semaphore_wait(barrier, K - 1)
            for to in mates:
                tell(ready_sem, to)

    drain(halo, halo_recv)
    for d in range(1, S):
        copy(places.at[sl], places.at[sl], place_send, place_recv, (me, space(d)))
        copy(early.at[sl], early.at[sl], early_send, early_recv, (me, space(d)))

    def u(a, i):
        if i < 2:
            return halo[0, a, CX - 2 + i]
        if i < 2 + CX:
            return ens[0, a, i - 2]
        return halo[1, a, i - 2 - CX]

    mids = range(1, CX + 3)
    for i in mids:
        rate, size = strain(*[[u(a, i + s) for a in range(3)] for s in (-1, 0, 1)])
        for p in range(6):
            strided[p, i - 1] = size * rate[p]
    for x in range(CX):
        i = x + 2
        for a in range(3):
            px, pz = PLACE[a, 0], PLACE[a, 2]
            flats[(a * CX + x) * NY : (a * CX + x + 1) * NY, :] = (
                strided[px, i] - strided[px, i - 2] + dz(strided[pz, i - 1])
            )
    along_y = jnp.concatenate(
        [strided[PLACE[a, 1], x + 1] for a in range(3) for x in range(CX)], axis=0
    )
    found = of_lanes(flats[...])
    first = of_rows(found, here)
    found = of_lanes(along_y)
    first = first + of_rows(found, after)
    second = of_rows(found, before)
    for i in mids:
        for a in range(3):
            smooth[a, i - 1] = filt(u(a, i - 1), u(a, i), u(a, i + 1))
    numer = jnp.zeros((NY, NZ), F32)
    denom = jnp.zeros((NY, NZ), F32)
    for i in range(2, CX + 2):
        rate, size = strain(*[[smooth[a, i - 1 + s] for a in range(3)] for s in (-1, 0, 1)])
        for p, (a, b) in enumerate(PAIRS):
            prod = filt(*[u(a, i + s) * u(b, i + s) for s in (-1, 0, 1)])
            leonard = prod - smooth[a, i - 1] * smooth[b, i - 1]
            model = 2.0 * (
                filt(strided[p, i - 2], strided[p, i - 1], strided[p, i]) - 4.0 * size * rate[p]
            )
            numer = numer + WEIGHTS[p] * (leonard * model)
            denom = denom + WEIGHTS[p] * (model * model)
    tiles = NY // 8
    row_8 = lax.broadcasted_iota(jnp.int32, (8, 128), 0)
    lane_8 = lax.broadcasted_iota(jnp.int32, (8, 128), 1)
    planes = []
    for v in (numer, denom):
        packed = jnp.zeros((8, 128), F32)
        for j in range(tiles):
            total = jnp.sum(v[j * 8 : j * 8 + 8], axis=1, keepdims=True)
            packed = jnp.where(lane_8 == j, total, packed)
        packed = gather_lanes(packed, lane_8 // 8)
        packed = jnp.where(lax.rem(lane_8, 8) == row_8, packed, 0.0)
        planes.append(jnp.sum(packed, axis=0, keepdims=True))
    late[sl, 0] = tile_of(first)
    late[sl, 1] = tile_of(second + planes)
    if short:

        @pl.when(hub)
        def _():
            pl.semaphore_wait(ready_sem, K - 1)

    for d in range(1, S):
        copy(late.at[sl], late.at[sl], late_send, late_recv, (me, space(d)))

    drain(early.at[0 : S - 1], early_recv)
    drain(places.at[0 : S - 1], place_recv)
    drain(late.at[0 : S - 1], late_recv)

    count = float(CX * S * NZ)
    above, below = [
        sum(jnp.broadcast_to(late[s, 1, NB + q : NB + q + 1, :], (T, 128)) for s in range(S))
        for q in range(2)
    ]
    ratio = jnp.where(lane_t < NY, (above / count) / (below / count + 1e-06), 0.0)
    quarter = 0.25 * ratio
    values = []
    for s in range(S):
        y = places[s]
        ya = jnp.where(row_t < NB, y, y + 1)
        yb = jnp.maximum(y - 1, 0)
        v = late[s, 0] * gather_lanes(quarter, ya)
        v = v - jnp.where(row_t < NB, late[s, 1] * gather_lanes(quarter, yb), 0.0)
        values.append(v + pltpu.roll(v, NB, 0) + early[s])
    own = pl.ds(pl.multiple_of(me * NH, 8), NH)
    hx[own, :] = jnp.concatenate(
        [jnp.where(row_t < NB, values[s], values[s + 1]) for s in range(0, S, 2)], axis=0
    )
    for d in range(K - 1, 0, -1):
        copy(hx.at[own], hx.at[own], hx_send, hx_recv, (mate(d), sl))

    coeff = jnp.concatenate(
        [gather_lanes(ratio[0:8], 8 * j + row_8) for j in range(tiles)], axis=0
    )
    per_layer = NY // RR
    for x in range(CX):
        for a in range(3):
            flat = flats[(a * CX + x) * NY : (a * CX + x + 1) * NY, :]
            term = coeff * flat + dy(coeff * strided[PLACE[a, 1], x + 1])
            f = ens[0, a, x] + 0.25 * term
            for t in range(per_layer):
                p = x * per_layer + t
                outbound[p, a * RR : (a + 1) * RR, :] = f[t * RR : (t + 1) * RR, :]
    for d in range(K - 1, 0, -1):
        copy(outbound.at[mate(d)], block.at[me], fwd_send, fwd_recv, (mate(d), sl))
    block[me] = outbound[me]

    drain(hx.at[pl.ds(0, (K - 1) * NH)], hx_recv)

    KK = K * K
    pair = max(1, 16 // K)
    fused = C % 128 == 0

    def slab_sum(s, acc):
        for b in range(NB):
            h = hx[pl.ds(s * NB + b, K, stride=NH), :]
            mean = jnp.sum(h, axis=0, keepdims=True) * (1.0 / K)
            anomaly = h - mean
            at = pl.ds(s * NB + b, 1)
            scaled = anomaly * (precision[at, :] * (1.0 / LEVELS))
            innov = value[at, :] - mean
            span = slice(b * 128, (b + 1) * 128)
            for m in range(0, K, pair):
                v = jnp.concatenate([anomaly[q : q + 1, :] * scaled for q in range(m, m + pair)], axis=0)
                hi, lo = split2(v)
                gmat[m * K : (m + pair) * K, span] = hi
                gmat[KK + m * K : KK + (m + pair) * K, span] = lo
            v = scaled * innov
            hi = v.astype(BF16).astype(F32)
            gmat[2 * KK :, span] = jnp.concatenate([hi, v - hi], axis=0).astype(BF16)
        span = pl.ds(pl.multiple_of(s * nob, 128), nob)
        g = gmat[...]
        if fused:
            return acc + lax.dot_general(g, parts[:, span], NT, preferred_element_type=F32)
        for q in range(2):
            acc = acc + lax.dot_general(
                g, parts[q * C : (q + 1) * C, span], NT, preferred_element_type=F32
            )
        return acc

    total = jnp.zeros((2 * (KK + K), 2 * C if fused else C), F32)
    if S <= 4:
        for s in range(S):
            total = slab_sum(s, total)
    else:
        total = lax.fori_loop(0, S, slab_sum, total)
    if fused:
        total = total[:, :C] + total[:, C:]
    amat = total[:KK] + total[KK : 2 * KK]
    drive = total[2 * KK : 2 * KK + K] + total[2 * KK + K :]
    if K <= 8:
        weights = transform_small(amat, drive, K, C)
    else:
        weights = transform_large(amat, drive, K, C, zr, yr, tr, ur)

    narrow = split2(jnp.concatenate(weights, axis=0))
    if fused:
        wide = jnp.dot(jnp.concatenate(narrow, axis=1), expand[...], preferred_element_type=F32)
    else:
        wide = sum(jnp.dot(v, expand[0:C, :], preferred_element_type=F32) for v in narrow)
    drain(block.at[0 : K - 1], fwd_recv)
    states = [block[m] for m in range(K)]
    centre = sum(states) * (1.0 / K)
    spread = [v - centre for v in states]
    for a in range(3):
        for r in range(RR):
            row = a * RR + r
            z0 = (r // CHUNK_Y) * NZ
            acc = jnp.broadcast_to(centre[row : row + 1, :], (K, NZ))
            for m in range(K):
                acc = acc + spread[m][row : row + 1, :] * wide[m * K : (m + 1) * K, z0 : z0 + NZ]
            result[pl.ds(row, K, stride=RP), :] = acc

    def of(k):
        return pl.ds(pl.multiple_of(k * RP, 8), RP)

    for d in range(K - 1, 0, -1):
        copy(result.at[of(mate(d))], back.at[me], ret_send, ret_recv, (mate(d), sl))
    back[me] = result[of(me), :]
    drain(back.at[0 : K - 1], ret_recv)
    for p in range(K):
        x, y0 = p // per_layer, (p % per_layer) * RR
        for a in range(3):
            out[0, a, x, y0 : y0 + RR, :] = back[p, a * RR : (a + 1) * RR, :]
    drain(halo, halo_send)
    drain(places.at[0 : S - 1], place_send)
    drain(early.at[0 : S - 1], early_send)
    drain(late.at[0 : S - 1], late_send)
    drain(hx.at[pl.ds(0, (K - 1) * NH)], hx_send)
    drain(block.at[0 : K - 1], fwd_send)
    drain(back.at[0 : K - 1], ret_send)


def solution(mesh):
    K, S = mesh.shape["member"], mesh.shape["space"]

    def shards(ensemble, obs_cell, obs_comp, obs_value, obs_precision, loc_obs, loc_level):
        CX, NY, NZ = ensemble.shape[2:]
        C = loc_obs.shape[0]
        NOBS = obs_value.shape[0]
        nob = obs_cell.shape[0]
        NB = nob // 128
        NH = NOBS // 128
        RR = CX * NY // K
        RP = -(-3 * RR // 8) * 8
        KK = K * K + K
        T = 2 * NB
        dims = (K, S, CX, NY, NZ, C, NOBS, RR, RP)
        large = (K, K, C) if K > 8 else (1, 8, 128)
        dma = pltpu.SemaphoreType.DMA
        vmem = pl.BlockSpec(memory_space=pltpu.VMEM)
        return pl.pallas_call(
            functools.partial(kernel, dims),
            out_shape=pltpu.VMEM(ensemble.shape, F32),
            in_specs=[pl.BlockSpec(memory_space=pl.ANY)] * 8,
            out_specs=vmem,
            scratch_shapes=[
                pltpu.VMEM(ensemble.shape, F32),
                pltpu.VMEM((1, nob), jnp.int32),
                pltpu.VMEM((NB, 128), jnp.int32),
                pltpu.VMEM((1, nob), jnp.int32),
                pltpu.VMEM((NH, 128), F32),
                pltpu.VMEM((NH, 128), F32),
                pltpu.VMEM((2, *loc_obs.shape), jnp.int32),
                dma((8,)),
                pltpu.VMEM((2, 3, CX, NY, NZ), F32),
                pltpu.VMEM((6, CX + 2, NY, NZ), F32),
                pltpu.VMEM((3, CX + 2, NY, NZ), F32),
                pltpu.VMEM((3 * CX * NY, NZ), F32),
                pltpu.VMEM((S, T, 128), F32),
                pltpu.VMEM((S, T, 128), jnp.int32),
                pltpu.VMEM((S, 2, T, 128), F32),
                pltpu.VMEM((K, RP, NZ), F32),
                pltpu.VMEM((K, RP, NZ), F32),
                pltpu.VMEM((K * NH, 128), F32),
                pltpu.VMEM((K * RP, NZ), F32),
                pltpu.VMEM((K, RP, NZ), F32),
                pltpu.VMEM((GROUP * NH, 128), F32),
                pltpu.VMEM((2 * C, NOBS), BF16),
                pltpu.VMEM((2 * NZ, nob), BF16),
                pltpu.VMEM((2 * C, RR // CHUNK_Y * NZ), BF16),
                pltpu.VMEM((2 * KK, nob), BF16),
                pltpu.VMEM(large, F32),
                pltpu.VMEM(large, F32),
                pltpu.VMEM(large, F32),
                pltpu.VMEM(large, F32),
            ] + [dma] * 14 + [pltpu.SemaphoreType.REGULAR] * 4,
            compiler_params=pltpu.CompilerParams(
                collective_id=0, has_side_effects=True, vmem_limit_bytes=60000 * 1024
            ),
            name="analysis_step",
        )(
            ensemble,
            obs_cell.reshape(1, nob),
            obs_cell.reshape(NB, 128),
            obs_comp.reshape(1, nob),
            obs_value.reshape(NH, 128),
            obs_precision.reshape(NH, 128),
            loc_obs,
            loc_level,
        )

    from jax.sharding import PartitionSpec as P

    field = P("member", None, "space", None, None)
    local = P(("space", "member"), None)
    return jax.shard_map(
        shards,
        mesh=mesh,
        in_specs=(field, P("space"), P("space"), P(), P(), local, local),
        out_specs=field,
        check_vma=False,
    )
```

```python
import functools

import jax
import jax.numpy as jnp
from jax import lax
from jax.experimental import pallas as pl
from jax.experimental.pallas import tpu as pltpu

NS_ITERS = 8
LEVELS = 8
CHUNK_Y = 3
CHUNK_Z = 4
GROUP = 16
PAIRS = ((0, 0), (1, 1), (2, 2), (0, 1), (0, 2), (1, 2))
WEIGHTS = (1.0, 1.0, 1.0, 2.0, 2.0, 2.0)
PLACE = {}
for _i, (_a, _b) in enumerate(PAIRS):
    PLACE[_a, _b] = PLACE[_b, _a] = _i
MESH = pl.DeviceIdType.MESH
F32 = jnp.float32
BF16 = jnp.bfloat16
NT = (((1,), (1,)), ((), ()))
TN = (((0,), (0,)), ((), ()))


def split2(x):
    hi = x.astype(BF16)
    return hi, (x - hi.astype(F32)).astype(BF16)


def split3(x):
    hi = x.astype(BF16)
    rest = x - hi.astype(F32)
    mid = rest.astype(BF16)
    low = (rest - mid.astype(F32)).astype(BF16)
    return hi, mid, low


def drain(ref, sem):
    pltpu.make_async_copy(ref, ref, sem).wait()


def gather_lanes(table, index):
    return jnp.take_along_axis(table, index, axis=1)


def dz(f):
    return pltpu.roll(f, f.shape[1] - 1, 1) - pltpu.roll(f, 1, 1)


def dy(f):
    n = f.shape[0]
    row = lax.broadcasted_iota(jnp.int32, f.shape, 0)
    after = jnp.where(row == n - 1, 0.0, pltpu.roll(f, n - 1, 0))
    before = jnp.where(row == 0, 0.0, pltpu.roll(f, 1, 0))
    return after - before


def filt(a, b, c):
    t = a + 2.0 * b + c
    return 0.0625 * (pltpu.roll(t, 1, 1) + 2.0 * t + pltpu.roll(t, t.shape[1] - 1, 1))


def strain(below, here, above):
    gx = [above[a] - below[a] for a in range(3)]
    gy = [dy(here[a]) for a in range(3)]
    gz = [dz(here[a]) for a in range(3)]
    rate = [
        0.5 * gx[0],
        0.5 * gy[1],
        0.5 * gz[2],
        0.25 * (gy[0] + gx[1]),
        0.25 * (gz[0] + gx[2]),
        0.25 * (gz[1] + gy[2]),
    ]
    diag = rate[0] * rate[0] + rate[1] * rate[1] + rate[2] * rate[2]
    off = rate[3] * rate[3] + rate[4] * rate[4] + rate[5] * rate[5]
    return rate, jnp.sqrt(2.0 * (diag + 2.0 * off))


def total_of(terms):
    while len(terms) > 1:
        terms = [
            terms[i] + terms[i + 1] if i + 1 < len(terms) else terms[i]
            for i in range(0, len(terms), 2)
        ]
    return terms[0]


def products(left, right, k):
    return [total_of([left[m][j : j + 1, :] * right[j] for j in range(k)]) for m in range(k)]


def transform_small(amat, drive, k, cols):
    row = lax.broadcasted_iota(jnp.int32, (k, cols), 0)
    eye = [jnp.where(row == m, 1.0, 0.0).astype(F32) for m in range(k)]
    matrix = [amat[m * k : (m + 1) * k, :] + ((k - 1) / 1.1) * eye[m] for m in range(k)]
    scale = jnp.sqrt(jnp.sum(total_of([v * v for v in matrix]), axis=0, keepdims=True))
    inv_scale = 1.0 / scale
    root = [v * inv_scale for v in matrix]
    inverse = eye
    for sweep in range(NS_ITERS):
        zy = products(inverse, root, k) if sweep else root
        factor = [1.5 * eye[m] - 0.5 * zy[m] for m in range(k)]
        if sweep < NS_ITERS - 1:
            root = products(factor, root, k)
        inverse = products(factor, inverse, k) if sweep else factor
    cover = products(inverse, inverse, k)
    gain = jnp.sqrt(k - 1.0) / jnp.sqrt(scale)
    out = []
    for m in range(k):
        wbar = jnp.sum(cover[m] * drive, axis=0, keepdims=True) * inv_scale
        out.append(gain * inverse[m] + wbar)
    return out


def transform_large(amat, drive, k, cols, zr, yr, tr, ur):
    def each(fn):
        lax.fori_loop(0, k, lambda m, c: (fn(m), c)[1], 0)

    row = lax.broadcasted_iota(jnp.int32, (k, cols), 0)

    def eye(m):
        return jnp.where(row == m, 1.0, 0.0).astype(F32)

    def product(left, right, out, post):
        def one(m):
            def step(j, acc):
                return acc + left[m, pl.ds(j, 1), :] * right[j]

            out[m] = post(m, lax.fori_loop(0, k, step, jnp.zeros((k, cols), F32)))

        each(one)

    for m in range(k):
        yr[m] = amat[m * k : (m + 1) * k, :] + ((k - 1) / 1.1) * eye(m)
        zr[m] = eye(m)
    total = lax.fori_loop(0, k, lambda m, a: a + yr[m] * yr[m], jnp.zeros((k, cols), F32))
    scale = jnp.sqrt(jnp.sum(total, axis=0, keepdims=True))

    def shrink(m):
        yr[m] = yr[m] / scale

    each(shrink)

    def same(m, v):
        return v

    def copy(src, dst):
        def one(m):
            dst[m] = src[m]

        each(one)

    def sweep(i, c):
        product(zr, yr, tr, lambda m, v: 1.5 * eye(m) - 0.5 * v)
        product(yr, tr, ur, same)
        copy(ur, yr)
        product(tr, zr, ur, same)
        copy(ur, zr)
        return c

    lax.fori_loop(0, NS_ITERS, sweep, 0)
    product(zr, zr, ur, same)
    gain = jnp.sqrt(k - 1.0) / jnp.sqrt(scale)
    return [
        gain * zr[m] + jnp.sum(ur[m] * drive, axis=0, keepdims=True) / scale for m in range(k)
    ]


def kernel(
    dims,
    ens_hbm, cell_hbm, tile_hbm, comp_hbm, value_hbm, precision_hbm, loc_hbm, level_hbm, out,
    ens, cell, cells2, comp, value, precision, local, load_sem,
    halo, strided, smooth, flats, early, places, late, outbound, block, hx, result, back,
    hist, parts, pick, expand, gmat, zr, yr, tr, ur,
    halo_send, halo_recv, early_send, early_recv, place_send, place_recv,
    late_send, late_recv, hx_send, hx_recv, fwd_send, fwd_recv, ret_send, ret_recv, near_sem, mid_sem, far_sem, ready_sem,
):
    K, S, CX, NY, NZ, C, NOBS, RR, RP = dims
    me = lax.axis_index("member")
    sl = lax.axis_index("space")
    nob = NOBS // S
    NB = nob // 128
    NH = NOBS // 128
    R = 3 * CX * NY
    T = 2 * NB
    short = S == 4

    def mate(d):
        bit, to = 1, me
        while bit < K:
            if d // bit % 2:
                to = to + bit - 2 * bit * lax.rem(me // bit, 2)
            bit *= 2
        return to

    def space(d):
        return lax.rem(sl + d, S)

    barrier = pltpu.get_barrier_semaphore()
    mates = [(mate(a), sl) for a in range(K - 1, 0, -1)]
    columns = [(me, space(b)) for b in range(1, S)]

    def tell(sem, to):
        pl.semaphore_signal(sem, inc=1, device_id=to, device_id_type=MESH)

    if short:
        root = sl == 0

        @pl.when(root)
        def _():
            tell(barrier, (me, space(1)))
            tell(barrier, (me, space(S - 1)))
            for to in mates:
                tell(barrier, to)

        @pl.when(sl == 1)
        def _():
            tell(barrier, (me, space(1)))

        @pl.when(sl > 1)
        def _():
            tell(barrier, (me, space(S - 1)))

    else:
        for to in columns + mates:
            tell(barrier, to)
    if short:

        @pl.when(sl > 0)
        def _():
            pl.semaphore_wait(barrier, jnp.where(sl == S - 1, 1, 2))

        @pl.when(sl == 1)
        def _():
            tell(near_sem, (me, 0 * sl))

        @pl.when(sl == S - 2)
        def _():
            tell(mid_sem, (me, space(1)))

        @pl.when(sl == S - 1)
        def _():
            tell(far_sem, (me, 0 * sl))

    else:
        pl.semaphore_wait(barrier, S - 1 + len(mates))

    loads = [
        pltpu.make_async_copy(src, dst, load_sem.at[i])
        for i, (src, dst) in enumerate(
            ((cell_hbm, cell), (tile_hbm, cells2), (comp_hbm, comp), (ens_hbm, ens),
             (loc_hbm, local.at[0]), (level_hbm, local.at[1]), (value_hbm, value), (precision_hbm, precision))
        )
    ]
    for c in loads:
        c.start()

    def copy(src, dst, send, recv, to):
        pltpu.make_async_remote_copy(
            src_ref=src, dst_ref=dst, send_sem=send, recv_sem=recv, device_id=to, device_id_type=MESH
        ).start()

    def up(*at):
        copy(ens_hbm.at[0, *at], halo.at[0, *at], halo_send, halo_recv, (me, space(1)))

    def down():
        copy(ens_hbm.at[0], halo.at[1], halo_send, halo_recv, (me, space(S - 1)))

    if short:

        @pl.when(root)
        def _():
            pl.semaphore_wait(near_sem, 1)

            @pl.when(lax.rem(me, 2) == 0)
            def _():
                up(0)
                pl.semaphore_wait(far_sem, 1)
                down()
                up(slice(1, 3))

            @pl.when(lax.rem(me, 2) == 1)
            def _():
                up()
                pl.semaphore_wait(far_sem, 1)
                down()

        @pl.when(sl > 0)
        def _():
            up()

            @pl.when(sl == S - 1)
            def _():
                pl.semaphore_wait(mid_sem, 1)

            down()
    else:
        up()
        down()
    for c in loads:
        c.wait()

    row_t = lax.broadcasted_iota(jnp.int32, (T, 128), 0)
    lane_t = lax.broadcasted_iota(jnp.int32, (T, 128), 1)
    cells = cell[...]
    lanes = lax.rem(cells, NZ)
    levels = cells // NZ
    heights = lax.rem(levels, NY)
    rows = comp[...] * (CX * NY) + levels
    iota_lane = lax.broadcasted_iota(jnp.int32, (NZ, nob), 0)
    one_hot = jnp.where(iota_lane == lanes, 1.0, 0.0).astype(BF16)
    pick[0:NZ, :] = one_hot
    pick[NZ:, :] = one_hot
    eighth = lax.broadcasted_iota(jnp.int32, (8, nob), 0)
    here = rows - eighth
    after = jnp.where(heights == NY - 1, -R, rows + 1) - eighth
    before = jnp.where(heights == 0, -R, rows - 1) - eighth

    def of_lanes(field):
        return jnp.dot(
            jnp.concatenate(split2(field), axis=1), pick[...], preferred_element_type=F32
        )

    def of_rows(found, wanted):
        acc = jnp.zeros((8, nob), F32)
        for t in range(R // 8):
            acc = acc + jnp.where(wanted == 8 * t, found[8 * t : 8 * t + 8, :], 0.0)
        seen = jnp.sum(acc, axis=0, keepdims=True)
        return [seen[:, b * 128 : (b + 1) * 128] for b in range(NB)]

    def tile_of(values):
        tile = jnp.zeros((T, 128), F32)
        for r, v in enumerate(values):
            tile = jnp.where(row_t == r, v, tile)
        return tile

    at_cells = lax.rem(cells2[...] // NZ, NY)
    places[sl] = jnp.concatenate([at_cells, at_cells], axis=0)
    fields = jnp.concatenate([ens[0, a, x] for a in range(3) for x in range(CX)], axis=0)
    found = sum(
        jnp.dot(v, pick[0:NZ, :], preferred_element_type=F32) for v in split3(fields)
    )
    seen = of_rows(found, here)
    early[sl] = tile_of(seen + seen)

    iota_hi = lax.broadcasted_iota(jnp.int32, (NH, 128), 0)
    iota_lo = lax.broadcasted_iota(jnp.int32, (128, 128), 0)

    def group(g, carry):
        base = pl.multiple_of(g * GROUP, GROUP)
        index = local[0, pl.ds(base, GROUP), :]
        weight = local[1, pl.ds(base, GROUP), :].astype(F32)
        top = lax.shift_right_logical(index, 7)
        low = jnp.bitwise_and(index, 127)
        for j in range(GROUP):
            a = jnp.where(iota_hi == top[j : j + 1, :], weight[j : j + 1, :], 0.0).astype(BF16)
            b = jnp.where(iota_lo == low[j : j + 1, :], 1.0, 0.0).astype(BF16)
            hist[j * NH : (j + 1) * NH, :] = lax.dot_general(a, b, NT, preferred_element_type=F32)
        for h in range(NH):
            big, small = split2(hist[pl.ds(h, GROUP, stride=NH), :])
            parts[pl.ds(base, GROUP), h * 128 : (h + 1) * 128] = big
            parts[pl.ds(C + base, GROUP), h * 128 : (h + 1) * 128] = small
        return carry

    lax.fori_loop(0, C // GROUP, group, 0)

    blocks_z = NZ // CHUNK_Z
    groups = RR // CHUNK_Y
    ci = lax.broadcasted_iota(jnp.int32, (C, groups * NZ), 0)
    zi = lax.broadcasted_iota(jnp.int32, (C, groups * NZ), 1)
    spread_z = jnp.where(ci == zi // CHUNK_Z, 1.0, 0.0).astype(BF16)
    expand[0:C, :] = spread_z
    expand[C:, :] = spread_z

    if short:

        @pl.when(root)
        def _():
            pl.semaphore_wait(barrier, K - 1)
            for to in mates:
                tell(ready_sem, to)

    drain(halo, halo_recv)
    for d in range(1, S):
        copy(places.at[sl], places.at[sl], place_send, place_recv, (me, space(d)))
        copy(early.at[sl], early.at[sl], early_send, early_recv, (me, space(d)))

    def u(a, i):
        if i < 2:
            return halo[0, a, CX - 2 + i]
        if i < 2 + CX:
            return ens[0, a, i - 2]
        return halo[1, a, i - 2 - CX]

    mids = range(1, CX + 3)
    for i in mids:
        rate, size = strain(*[[u(a, i + s) for a in range(3)] for s in (-1, 0, 1)])
        for p in range(6):
            strided[p, i - 1] = size * rate[p]
    for x in range(CX):
        i = x + 2
        for a in range(3):
            px, pz = PLACE[a, 0], PLACE[a, 2]
            flats[(a * CX + x) * NY : (a * CX + x + 1) * NY, :] = (
                strided[px, i] - strided[px, i - 2] + dz(strided[pz, i - 1])
            )
    along_y = jnp.concatenate(
        [strided[PLACE[a, 1], x + 1] for a in range(3) for x in range(CX)], axis=0
    )
    found = of_lanes(flats[...])
    first = of_rows(found, here)
    found = of_lanes(along_y)
    first = first + of_rows(found, after)
    second = of_rows(found, before)
    for i in mids:
        for a in range(3):
            smooth[a, i - 1] = filt(u(a, i - 1), u(a, i), u(a, i + 1))
    numer = jnp.zeros((NY, NZ), F32)
    denom = jnp.zeros((NY, NZ), F32)
    for i in range(2, CX + 2):
        rate, size = strain(*[[smooth[a, i - 1 + s] for a in range(3)] for s in (-1, 0, 1)])
        for p, (a, b) in enumerate(PAIRS):
            prod = filt(*[u(a, i + s) * u(b, i + s) for s in (-1, 0, 1)])
            leonard = prod - smooth[a, i - 1] * smooth[b, i - 1]
            model = 2.0 * (
                filt(strided[p, i - 2], strided[p, i - 1], strided[p, i]) - 4.0 * size * rate[p]
            )
            numer = numer + WEIGHTS[p] * (leonard * model)
            denom = denom + WEIGHTS[p] * (model * model)
    tiles = NY // 8
    row_8 = lax.broadcasted_iota(jnp.int32, (8, 128), 0)
    lane_8 = lax.broadcasted_iota(jnp.int32, (8, 128), 1)
    planes = []
    for v in (numer, denom):
        packed = jnp.zeros((8, 128), F32)
        for j in range(tiles):
            total = jnp.sum(v[j * 8 : j * 8 + 8], axis=1, keepdims=True)
            packed = jnp.where(lane_8 == j, total, packed)
        packed = gather_lanes(packed, lane_8 // 8)
        packed = jnp.where(lax.rem(lane_8, 8) == row_8, packed, 0.0)
        planes.append(jnp.sum(packed, axis=0, keepdims=True))
    late[sl, 0] = tile_of(first)
    late[sl, 1] = tile_of(second + planes)
    if short:

        @pl.when(root)
        def _():
            pl.semaphore_wait(ready_sem, K - 1)

    for d in range(1, S):
        copy(late.at[sl], late.at[sl], late_send, late_recv, (me, space(d)))

    drain(early.at[0 : S - 1], early_recv)
    drain(places.at[0 : S - 1], place_recv)
    drain(late.at[0 : S - 1], late_recv)

    count = float(CX * S * NZ)
    above, below = [
        sum(jnp.broadcast_to(late[s, 1, NB + q : NB + q + 1, :], (T, 128)) for s in range(S))
        for q in range(2)
    ]
    ratio = jnp.where(lane_t < NY, (above / count) / (below / count + 1e-06), 0.0)
    quarter = 0.25 * ratio
    values = []
    for s in range(S):
        y = places[s]
        ya = jnp.where(row_t < NB, y, y + 1)
        yb = jnp.maximum(y - 1, 0)
        v = late[s, 0] * gather_lanes(quarter, ya)
        v = v - jnp.where(row_t < NB, late[s, 1] * gather_lanes(quarter, yb), 0.0)
        values.append(v + pltpu.roll(v, NB, 0) + early[s])
    own = pl.ds(pl.multiple_of(me * NH, 8), NH)
    hx[own, :] = jnp.concatenate(
        [jnp.where(row_t < NB, values[s], values[s + 1]) for s in range(0, S, 2)], axis=0
    )
    for d in range(K - 1, 0, -1):
        copy(hx.at[own], hx.at[own], hx_send, hx_recv, (mate(d), sl))

    coeff = jnp.concatenate(
        [gather_lanes(ratio[0:8], 8 * j + row_8) for j in range(tiles)], axis=0
    )
    per_layer = NY // RR
    for x in range(CX):
        for a in range(3):
            flat = flats[(a * CX + x) * NY : (a * CX + x + 1) * NY, :]
            term = coeff * flat + dy(coeff * strided[PLACE[a, 1], x + 1])
            f = ens[0, a, x] + 0.25 * term
            for t in range(per_layer):
                p = x * per_layer + t
                outbound[p, a * RR : (a + 1) * RR, :] = f[t * RR : (t + 1) * RR, :]
    for d in range(K - 1, 0, -1):
        copy(outbound.at[mate(d), 0 : 3 * RR], block.at[me, 0 : 3 * RR], fwd_send, fwd_recv, (mate(d), sl))
    block[me] = outbound[me]

    drain(hx.at[pl.ds(0, (K - 1) * NH)], hx_recv)

    KK = K * K
    pair = max(1, 16 // K)
    fused = C % 128 == 0

    def slab_rows(s, start):
        for b in range(NB):
            h = hx[pl.ds(s * NB + b, K, stride=NH), :]
            mean = jnp.sum(h, axis=0, keepdims=True) * (1.0 / K)
            anomaly = h - mean
            at = pl.ds(s * NB + b, 1)
            scaled = anomaly * (precision[at, :] * (1.0 / LEVELS))
            innov = value[at, :] - mean
            span = slice(start + b * 128, start + (b + 1) * 128)
            for m in range(0, K, pair):
                v = jnp.concatenate([anomaly[q : q + 1, :] * scaled for q in range(m, m + pair)], axis=0)
                hi, lo = split2(v)
                gmat[m * K : (m + pair) * K, span] = hi
                gmat[KK + m * K : KK + (m + pair) * K, span] = lo
            v = scaled * innov
            hi = v.astype(BF16).astype(F32)
            gmat[2 * KK :, span] = jnp.concatenate([hi, v - hi], axis=0).astype(BF16)

    def against(span):
        g = gmat[...]
        if fused:
            return lax.dot_general(g, parts[:, span], NT, preferred_element_type=F32)
        return sum(
            lax.dot_general(g, parts[q * C : (q + 1) * C, span], NT, preferred_element_type=F32)
            for q in range(2)
        )

    def slab_sum(s, acc):
        slab_rows(s, 0)
        return acc + against(pl.ds(pl.multiple_of(s * nob, 128), nob))

    if S <= 4:
        for s in range(S):
            slab_rows(s, s * nob)
        total = against(slice(0, NOBS))
    else:
        total = jnp.zeros((2 * (KK + K), 2 * C if fused else C), F32)
        total = lax.fori_loop(0, S, slab_sum, total)
    if fused:
        total = total[:, :C] + total[:, C:]
    amat = total[:KK] + total[KK : 2 * KK]
    drive = total[2 * KK : 2 * KK + K] + total[2 * KK + K :]
    if K <= 8:
        weights = transform_small(amat, drive, K, C)
    else:
        weights = transform_large(amat, drive, K, C, zr, yr, tr, ur)

    narrow = split2(jnp.concatenate(weights, axis=0))
    if fused:
        wide = jnp.dot(jnp.concatenate(narrow, axis=1), expand[...], preferred_element_type=F32)
    else:
        wide = sum(jnp.dot(v, expand[0:C, :], preferred_element_type=F32) for v in narrow)
    drain(block.at[0 : K - 1, 0 : 3 * RR], fwd_recv)
    states = [block[m] for m in range(K)]
    centre = sum(states) * (1.0 / K)
    spread = [v - centre for v in states]
    for a in range(3):
        for r in range(RR):
            row = a * RR + r
            z0 = (r // CHUNK_Y) * NZ
            acc = jnp.broadcast_to(centre[row : row + 1, :], (K, NZ))
            for m in range(K):
                acc = acc + spread[m][row : row + 1, :] * wide[m * K : (m + 1) * K, z0 : z0 + NZ]
            result[pl.ds(row, K, stride=RP), :] = acc

    def of(k):
        return pl.ds(pl.multiple_of(k * RP, 8), 3 * RR)

    for d in range(K - 1, 0, -1):
        copy(result.at[of(mate(d))], back.at[me, 0 : 3 * RR], ret_send, ret_recv, (mate(d), sl))
    back[me, 0 : 3 * RR] = result[of(me), :]
    drain(back.at[0 : K - 1, 0 : 3 * RR], ret_recv)
    for p in range(K):
        x, y0 = p // per_layer, (p % per_layer) * RR
        for a in range(3):
            out[0, a, x, y0 : y0 + RR, :] = back[p, a * RR : (a + 1) * RR, :]
    drain(halo, halo_send)
    drain(places.at[0 : S - 1], place_send)
    drain(early.at[0 : S - 1], early_send)
    drain(late.at[0 : S - 1], late_send)
    drain(hx.at[pl.ds(0, (K - 1) * NH)], hx_send)
    drain(block.at[0 : K - 1, 0 : 3 * RR], fwd_send)
    drain(back.at[0 : K - 1, 0 : 3 * RR], ret_send)


def solution(mesh):
    K, S = mesh.shape["member"], mesh.shape["space"]

    def shards(ensemble, obs_cell, obs_comp, obs_value, obs_precision, loc_obs, loc_level):
        CX, NY, NZ = ensemble.shape[2:]
        C = loc_obs.shape[0]
        NOBS = obs_value.shape[0]
        nob = obs_cell.shape[0]
        NB = nob // 128
        NH = NOBS // 128
        RR = CX * NY // K
        RP = -(-3 * RR // 8) * 8
        KK = K * K + K
        T = 2 * NB
        dims = (K, S, CX, NY, NZ, C, NOBS, RR, RP)
        large = (K, K, C) if K > 8 else (1, 8, 128)
        dma = pltpu.SemaphoreType.DMA
        vmem = pl.BlockSpec(memory_space=pltpu.VMEM)
        return pl.pallas_call(
            functools.partial(kernel, dims),
            out_shape=pltpu.VMEM(ensemble.shape, F32),
            in_specs=[pl.BlockSpec(memory_space=pl.ANY)] * 8,
            out_specs=vmem,
            scratch_shapes=[
                pltpu.VMEM(ensemble.shape, F32),
                pltpu.VMEM((1, nob), jnp.int32),
                pltpu.VMEM((NB, 128), jnp.int32),
                pltpu.VMEM((1, nob), jnp.int32),
                pltpu.VMEM((NH, 128), F32),
                pltpu.VMEM((NH, 128), F32),
                pltpu.VMEM((2, *loc_obs.shape), jnp.int32),
                dma((8,)),
                pltpu.VMEM((2, 3, CX, NY, NZ), F32),
                pltpu.VMEM((6, CX + 2, NY, NZ), F32),
                pltpu.VMEM((3, CX + 2, NY, NZ), F32),
                pltpu.VMEM((3 * CX * NY, NZ), F32),
                pltpu.VMEM((S, T, 128), F32),
                pltpu.VMEM((S, T, 128), jnp.int32),
                pltpu.VMEM((S, 2, T, 128), F32),
                pltpu.VMEM((K, RP, NZ), F32),
                pltpu.VMEM((K, RP, NZ), F32),
                pltpu.VMEM((K * NH, 128), F32),
                pltpu.VMEM((K * RP, NZ), F32),
                pltpu.VMEM((K, RP, NZ), F32),
                pltpu.VMEM((GROUP * NH, 128), F32),
                pltpu.VMEM((2 * C, NOBS), BF16),
                pltpu.VMEM((2 * NZ, nob), BF16),
                pltpu.VMEM((2 * C, RR // CHUNK_Y * NZ), BF16),
                pltpu.VMEM((2 * KK, NOBS if S <= 4 else nob), BF16),
                pltpu.VMEM(large, F32),
                pltpu.VMEM(large, F32),
                pltpu.VMEM(large, F32),
                pltpu.VMEM(large, F32),
            ] + [dma] * 14 + [pltpu.SemaphoreType.REGULAR] * 4,
            compiler_params=pltpu.CompilerParams(
                collective_id=0, has_side_effects=True, vmem_limit_bytes=60000 * 1024
            ),
            name="analysis_step",
        )(
            ensemble,
            obs_cell.reshape(1, nob),
            obs_cell.reshape(NB, 128),
            obs_comp.reshape(1, nob),
            obs_value.reshape(NH, 128),
            obs_precision.reshape(NH, 128),
            loc_obs,
            loc_level,
        )

    from jax.sharding import PartitionSpec as P

    field = P("member", None, "space", None, None)
    local = P(("space", "member"), None)
    return jax.shard_map(
        shards,
        mesh=mesh,
        in_specs=(field, P("space"), P("space"), P(), P(), local, local),
        out_specs=field,
        check_vma=False,
    )
```

```python
import functools

import jax
import jax.numpy as jnp
from jax import lax
from jax.experimental import pallas as pl
from jax.experimental.pallas import tpu as pltpu

NS_ITERS = 8
LEVELS = 8
CHUNK_Y = 3
CHUNK_Z = 4
GROUP = 16
PAIRS = ((0, 0), (1, 1), (2, 2), (0, 1), (0, 2), (1, 2))
WEIGHTS = (1.0, 1.0, 1.0, 2.0, 2.0, 2.0)
PLACE = {}
for _i, (_a, _b) in enumerate(PAIRS):
    PLACE[_a, _b] = PLACE[_b, _a] = _i
MESH = pl.DeviceIdType.MESH
F32 = jnp.float32
BF16 = jnp.bfloat16
NT = (((1,), (1,)), ((), ()))
TN = (((0,), (0,)), ((), ()))


def split2(x):
    hi = x.astype(BF16)
    return hi, (x - hi.astype(F32)).astype(BF16)


def split3(x):
    hi = x.astype(BF16)
    rest = x - hi.astype(F32)
    mid = rest.astype(BF16)
    low = (rest - mid.astype(F32)).astype(BF16)
    return hi, mid, low


def drain(ref, sem):
    pltpu.make_async_copy(ref, ref, sem).wait()


def gather_lanes(table, index):
    return jnp.take_along_axis(table, index, axis=1)


def dz(f):
    return pltpu.roll(f, f.shape[1] - 1, 1) - pltpu.roll(f, 1, 1)


def dy(f):
    n = f.shape[0]
    row = lax.broadcasted_iota(jnp.int32, f.shape, 0)
    after = jnp.where(row == n - 1, 0.0, pltpu.roll(f, n - 1, 0))
    before = jnp.where(row == 0, 0.0, pltpu.roll(f, 1, 0))
    return after - before


def filt(a, b, c):
    t = a + 2.0 * b + c
    return 0.0625 * (pltpu.roll(t, 1, 1) + 2.0 * t + pltpu.roll(t, t.shape[1] - 1, 1))


def strain(below, here, above):
    gx = [above[a] - below[a] for a in range(3)]
    gy = [dy(here[a]) for a in range(3)]
    gz = [dz(here[a]) for a in range(3)]
    rate = [
        0.5 * gx[0],
        0.5 * gy[1],
        0.5 * gz[2],
        0.25 * (gy[0] + gx[1]),
        0.25 * (gz[0] + gx[2]),
        0.25 * (gz[1] + gy[2]),
    ]
    diag = rate[0] * rate[0] + rate[1] * rate[1] + rate[2] * rate[2]
    off = rate[3] * rate[3] + rate[4] * rate[4] + rate[5] * rate[5]
    return rate, jnp.sqrt(2.0 * (diag + 2.0 * off))


def total_of(terms):
    while len(terms) > 1:
        terms = [
            terms[i] + terms[i + 1] if i + 1 < len(terms) else terms[i]
            for i in range(0, len(terms), 2)
        ]
    return terms[0]


def turn(v, d):
    k = v.shape[0]
    return pltpu.roll(v, (k - d) % k, 0) if d % k else v


def turned(bands, k):
    memo = {}

    def band(g, d):
        if (g, d) not in memo:
            memo[g, d] = turn(bands[g], d)
        return memo[g, d]

    def entry(f, d):
        f, d = f % k, d % k
        return band(f, d) if f <= k // 2 else band(k - f, (d + f) % k)

    return entry


def product(left, right, k):
    x, y = turned(left, k), turned(right, k)
    return [
        total_of([x(d, 0) * y(e - d, d) for d in range(k)]) for e in range(k // 2 + 1)
    ]


def transform_bands(bands, drive, k):
    half = k // 2
    matrix = [bands[0] + (k - 1) / 1.1] + bands[1:]
    squares = [v * v for v in matrix]
    off = total_of(squares[1:half])
    scale = jnp.sqrt(jnp.sum(squares[0] + squares[half] + 2.0 * off, axis=0, keepdims=True))
    inv_scale = 1.0 / scale
    root = [v * inv_scale for v in matrix]
    inverse = None
    for sweep in range(NS_ITERS):
        zy = product(inverse, root, k) if sweep else root
        factor = [1.5 - 0.5 * zy[0]] + [-0.5 * v for v in zy[1:]]
        if sweep < NS_ITERS - 1:
            root = product(factor, root, k)
        inverse = product(factor, inverse, k) if sweep else factor
    z = turned(inverse, k)

    def times(v):
        return total_of([z(d, 0) * turn(v, d) for d in range(k)])

    wbar = times(times(drive)) * inv_scale
    gain = jnp.sqrt(k - 1.0) / jnp.sqrt(scale)
    bent = [gain * z(d, 0) + turn(wbar, d) for d in range(k)]
    row = lax.broadcasted_iota(jnp.int32, wbar.shape, 0)
    out = []
    for m in range(k):
        v = bent[0]
        for d in range(1, k):
            v = jnp.where(row == (m - d) % k, bent[d], v)
        out.append(v)
    return out


def transform_large(amat, drive, k, cols, zr, yr, tr, ur):
    def each(fn):
        lax.fori_loop(0, k, lambda m, c: (fn(m), c)[1], 0)

    row = lax.broadcasted_iota(jnp.int32, (k, cols), 0)

    def eye(m):
        return jnp.where(row == m, 1.0, 0.0).astype(F32)

    def product(left, right, out, post):
        def one(m):
            def step(j, acc):
                return acc + left[m, pl.ds(j, 1), :] * right[j]

            out[m] = post(m, lax.fori_loop(0, k, step, jnp.zeros((k, cols), F32)))

        each(one)

    for m in range(k):
        yr[m] = amat[m * k : (m + 1) * k, :] + ((k - 1) / 1.1) * eye(m)
        zr[m] = eye(m)
    total = lax.fori_loop(0, k, lambda m, a: a + yr[m] * yr[m], jnp.zeros((k, cols), F32))
    scale = jnp.sqrt(jnp.sum(total, axis=0, keepdims=True))

    def shrink(m):
        yr[m] = yr[m] / scale

    each(shrink)

    def same(m, v):
        return v

    def copy(src, dst):
        def one(m):
            dst[m] = src[m]

        each(one)

    def sweep(i, c):
        product(zr, yr, tr, lambda m, v: 1.5 * eye(m) - 0.5 * v)
        product(yr, tr, ur, same)
        copy(ur, yr)
        product(tr, zr, ur, same)
        copy(ur, zr)
        return c

    lax.fori_loop(0, NS_ITERS, sweep, 0)
    product(zr, zr, ur, same)
    gain = jnp.sqrt(k - 1.0) / jnp.sqrt(scale)
    return [
        gain * zr[m] + jnp.sum(ur[m] * drive, axis=0, keepdims=True) / scale for m in range(k)
    ]


def kernel(
    dims,
    ens_hbm, cell_hbm, tile_hbm, comp_hbm, value_hbm, precision_hbm, loc_hbm, level_hbm, out,
    ens, cell, cells2, comp, value, precision, local, load_sem,
    halo, strided, smooth, flats, early, places, late, outbound, block, hx, result, back,
    hist, parts, pick, expand, gmat, zr, yr, tr, ur,
    halo_send, halo_recv, early_send, early_recv, place_send, place_recv,
    late_send, late_recv, hx_send, hx_recv, fwd_send, fwd_recv, ret_send, ret_recv, near_sem, mid_sem, far_sem, ready_sem,
):
    K, S, CX, NY, NZ, C, NOBS, RR, RP = dims
    me = lax.axis_index("member")
    sl = lax.axis_index("space")
    nob = NOBS // S
    NB = nob // 128
    NH = NOBS // 128
    R = 3 * CX * NY
    T = 2 * NB
    short = S == 4

    def mate(d):
        bit, to = 1, me
        while bit < K:
            if d // bit % 2:
                to = to + bit - 2 * bit * lax.rem(me // bit, 2)
            bit *= 2
        return to

    def space(d):
        return lax.rem(sl + d, S)

    barrier = pltpu.get_barrier_semaphore()
    mates = [(mate(a), sl) for a in range(K - 1, 0, -1)]
    columns = [(me, space(b)) for b in range(1, S)]

    def tell(sem, to):
        pl.semaphore_signal(sem, inc=1, device_id=to, device_id_type=MESH)

    if short:
        root = sl == 0

        @pl.when(root)
        def _():
            tell(barrier, (me, space(1)))
            tell(barrier, (me, space(S - 1)))
            for to in mates:
                tell(barrier, to)

        @pl.when(sl == 1)
        def _():
            tell(barrier, (me, space(1)))

        @pl.when(sl > 1)
        def _():
            tell(barrier, (me, space(S - 1)))

    else:
        for to in columns + mates:
            tell(barrier, to)
    if short:

        @pl.when(sl > 0)
        def _():
            pl.semaphore_wait(barrier, jnp.where(sl == S - 1, 1, 2))

        @pl.when(sl == 1)
        def _():
            tell(near_sem, (me, 0 * sl))

        @pl.when(sl == S - 2)
        def _():
            tell(mid_sem, (me, space(1)))

        @pl.when(sl == S - 1)
        def _():
            tell(far_sem, (me, 0 * sl))

    else:
        pl.semaphore_wait(barrier, S - 1 + len(mates))

    loads = [
        pltpu.make_async_copy(src, dst, load_sem.at[i])
        for i, (src, dst) in enumerate(
            ((cell_hbm, cell), (tile_hbm, cells2), (comp_hbm, comp), (ens_hbm, ens),
             (loc_hbm, local.at[0]), (level_hbm, local.at[1]), (value_hbm, value), (precision_hbm, precision))
        )
    ]
    for c in loads:
        c.start()

    def copy(src, dst, send, recv, to):
        pltpu.make_async_remote_copy(
            src_ref=src, dst_ref=dst, send_sem=send, recv_sem=recv, device_id=to, device_id_type=MESH
        ).start()

    def up(*at):
        copy(ens_hbm.at[0, *at], halo.at[0, *at], halo_send, halo_recv, (me, space(1)))

    def down():
        copy(ens_hbm.at[0], halo.at[1], halo_send, halo_recv, (me, space(S - 1)))

    if short:

        @pl.when(root)
        def _():
            pl.semaphore_wait(near_sem, 1)

            @pl.when(lax.rem(me, 2) == 0)
            def _():
                up(0)
                pl.semaphore_wait(far_sem, 1)
                down()
                up(slice(1, 3))

            @pl.when(lax.rem(me, 2) == 1)
            def _():
                up()
                pl.semaphore_wait(far_sem, 1)
                down()

        @pl.when(sl > 0)
        def _():
            up()

            @pl.when(sl == S - 1)
            def _():
                pl.semaphore_wait(mid_sem, 1)

            down()
    else:
        up()
        down()
    for c in loads:
        c.wait()

    row_t = lax.broadcasted_iota(jnp.int32, (T, 128), 0)
    lane_t = lax.broadcasted_iota(jnp.int32, (T, 128), 1)
    cells = cell[...]
    lanes = lax.rem(cells, NZ)
    levels = cells // NZ
    heights = lax.rem(levels, NY)
    rows = comp[...] * (CX * NY) + levels
    iota_lane = lax.broadcasted_iota(jnp.int32, (NZ, nob), 0)
    one_hot = jnp.where(iota_lane == lanes, 1.0, 0.0).astype(BF16)
    pick[0:NZ, :] = one_hot
    pick[NZ:, :] = one_hot
    eighth = lax.broadcasted_iota(jnp.int32, (8, nob), 0)
    here = rows - eighth
    after = jnp.where(heights == NY - 1, -R, rows + 1) - eighth
    before = jnp.where(heights == 0, -R, rows - 1) - eighth

    def of_lanes(field):
        return jnp.dot(
            jnp.concatenate(split2(field), axis=1), pick[...], preferred_element_type=F32
        )

    def of_rows(found, wanted):
        acc = jnp.zeros((8, nob), F32)
        for t in range(R // 8):
            acc = acc + jnp.where(wanted == 8 * t, found[8 * t : 8 * t + 8, :], 0.0)
        seen = jnp.sum(acc, axis=0, keepdims=True)
        return [seen[:, b * 128 : (b + 1) * 128] for b in range(NB)]

    def tile_of(values):
        tile = jnp.zeros((T, 128), F32)
        for r, v in enumerate(values):
            tile = jnp.where(row_t == r, v, tile)
        return tile

    at_cells = lax.rem(cells2[...] // NZ, NY)
    places[sl] = jnp.concatenate([at_cells, at_cells], axis=0)
    fields = jnp.concatenate([ens[0, a, x] for a in range(3) for x in range(CX)], axis=0)
    found = sum(
        jnp.dot(v, pick[0:NZ, :], preferred_element_type=F32) for v in split3(fields)
    )
    seen = of_rows(found, here)
    early[sl] = tile_of(seen + seen)

    iota_hi = lax.broadcasted_iota(jnp.int32, (NH, 128), 0)
    iota_lo = lax.broadcasted_iota(jnp.int32, (128, 128), 0)

    def group(g, carry):
        base = pl.multiple_of(g * GROUP, GROUP)
        index = local[0, pl.ds(base, GROUP), :]
        weight = local[1, pl.ds(base, GROUP), :].astype(F32)
        top = lax.shift_right_logical(index, 7)
        low = jnp.bitwise_and(index, 127)
        for j in range(GROUP):
            a = jnp.where(iota_hi == top[j : j + 1, :], weight[j : j + 1, :], 0.0).astype(BF16)
            b = jnp.where(iota_lo == low[j : j + 1, :], 1.0, 0.0).astype(BF16)
            hist[j * NH : (j + 1) * NH, :] = lax.dot_general(a, b, NT, preferred_element_type=F32)
        for h in range(NH):
            big, small = split2(hist[pl.ds(h, GROUP, stride=NH), :])
            parts[pl.ds(base, GROUP), h * 128 : (h + 1) * 128] = big
            parts[pl.ds(C + base, GROUP), h * 128 : (h + 1) * 128] = small
        return carry

    lax.fori_loop(0, C // GROUP, group, 0)

    blocks_z = NZ // CHUNK_Z
    groups = RR // CHUNK_Y
    ci = lax.broadcasted_iota(jnp.int32, (C, groups * NZ), 0)
    zi = lax.broadcasted_iota(jnp.int32, (C, groups * NZ), 1)
    spread_z = jnp.where(ci == zi // CHUNK_Z, 1.0, 0.0).astype(BF16)
    expand[0:C, :] = spread_z
    expand[C:, :] = spread_z

    if short:

        @pl.when(root)
        def _():
            pl.semaphore_wait(barrier, K - 1)
            for to in mates:
                tell(ready_sem, to)

    drain(halo, halo_recv)
    for d in range(1, S):
        copy(places.at[sl], places.at[sl], place_send, place_recv, (me, space(d)))
        copy(early.at[sl], early.at[sl], early_send, early_recv, (me, space(d)))

    def u(a, i):
        if i < 2:
            return halo[0, a, CX - 2 + i]
        if i < 2 + CX:
            return ens[0, a, i - 2]
        return halo[1, a, i - 2 - CX]

    mids = range(1, CX + 3)
    for i in mids:
        rate, size = strain(*[[u(a, i + s) for a in range(3)] for s in (-1, 0, 1)])
        for p in range(6):
            strided[p, i - 1] = size * rate[p]
    for x in range(CX):
        i = x + 2
        for a in range(3):
            px, pz = PLACE[a, 0], PLACE[a, 2]
            flats[(a * CX + x) * NY : (a * CX + x + 1) * NY, :] = (
                strided[px, i] - strided[px, i - 2] + dz(strided[pz, i - 1])
            )
    along_y = jnp.concatenate(
        [strided[PLACE[a, 1], x + 1] for a in range(3) for x in range(CX)], axis=0
    )
    found = of_lanes(flats[...])
    first = of_rows(found, here)
    found = of_lanes(along_y)
    first = first + of_rows(found, after)
    second = of_rows(found, before)
    for i in mids:
        for a in range(3):
            smooth[a, i - 1] = filt(u(a, i - 1), u(a, i), u(a, i + 1))
    numer = jnp.zeros((NY, NZ), F32)
    denom = jnp.zeros((NY, NZ), F32)
    for i in range(2, CX + 2):
        rate, size = strain(*[[smooth[a, i - 1 + s] for a in range(3)] for s in (-1, 0, 1)])
        for p, (a, b) in enumerate(PAIRS):
            prod = filt(*[u(a, i + s) * u(b, i + s) for s in (-1, 0, 1)])
            leonard = prod - smooth[a, i - 1] * smooth[b, i - 1]
            model = 2.0 * (
                filt(strided[p, i - 2], strided[p, i - 1], strided[p, i]) - 4.0 * size * rate[p]
            )
            numer = numer + WEIGHTS[p] * (leonard * model)
            denom = denom + WEIGHTS[p] * (model * model)
    tiles = NY // 8
    row_8 = lax.broadcasted_iota(jnp.int32, (8, 128), 0)
    lane_8 = lax.broadcasted_iota(jnp.int32, (8, 128), 1)
    planes = []
    for v in (numer, denom):
        packed = jnp.zeros((8, 128), F32)
        for j in range(tiles):
            total = jnp.sum(v[j * 8 : j * 8 + 8], axis=1, keepdims=True)
            packed = jnp.where(lane_8 == j, total, packed)
        packed = gather_lanes(packed, lane_8 // 8)
        packed = jnp.where(lax.rem(lane_8, 8) == row_8, packed, 0.0)
        planes.append(jnp.sum(packed, axis=0, keepdims=True))
    late[sl, 0] = tile_of(first)
    late[sl, 1] = tile_of(second + planes)
    if short:

        @pl.when(root)
        def _():
            pl.semaphore_wait(ready_sem, K - 1)

    for d in range(1, S):
        copy(late.at[sl], late.at[sl], late_send, late_recv, (me, space(d)))

    drain(early.at[0 : S - 1], early_recv)
    drain(places.at[0 : S - 1], place_recv)
    drain(late.at[0 : S - 1], late_recv)

    count = float(CX * S * NZ)
    above, below = [
        sum(jnp.broadcast_to(late[s, 1, NB + q : NB + q + 1, :], (T, 128)) for s in range(S))
        for q in range(2)
    ]
    ratio = jnp.where(lane_t < NY, (above / count) / (below / count + 1e-06), 0.0)
    quarter = 0.25 * ratio
    values = []
    for s in range(S):
        y = places[s]
        ya = jnp.where(row_t < NB, y, y + 1)
        yb = jnp.maximum(y - 1, 0)
        v = late[s, 0] * gather_lanes(quarter, ya)
        v = v - jnp.where(row_t < NB, late[s, 1] * gather_lanes(quarter, yb), 0.0)
        values.append(v + pltpu.roll(v, NB, 0) + early[s])
    own = pl.ds(pl.multiple_of(me * NH, 8), NH)
    hx[own, :] = jnp.concatenate(
        [jnp.where(row_t < NB, values[s], values[s + 1]) for s in range(0, S, 2)], axis=0
    )
    for d in range(K - 1, 0, -1):
        copy(hx.at[own], hx.at[own], hx_send, hx_recv, (mate(d), sl))

    coeff = jnp.concatenate(
        [gather_lanes(ratio[0:8], 8 * j + row_8) for j in range(tiles)], axis=0
    )
    per_layer = NY // RR
    for x in range(CX):
        for a in range(3):
            flat = flats[(a * CX + x) * NY : (a * CX + x + 1) * NY, :]
            term = coeff * flat + dy(coeff * strided[PLACE[a, 1], x + 1])
            f = ens[0, a, x] + 0.25 * term
            for t in range(per_layer):
                p = x * per_layer + t
                outbound[p, a * RR : (a + 1) * RR, :] = f[t * RR : (t + 1) * RR, :]
    for d in range(K - 1, 0, -1):
        copy(outbound.at[mate(d), 0 : 3 * RR], block.at[me, 0 : 3 * RR], fwd_send, fwd_recv, (mate(d), sl))
    block[me] = outbound[me]

    drain(hx.at[pl.ds(0, (K - 1) * NH)], hx_recv)

    KK = K * K
    pair = max(1, 16 // K)
    banded = K == 8
    half_rows = (K // 2 + 2) * K if banded else KK + K
    assert half_rows // K % pair == 0
    fused = C % 128 == 0

    def fill(first_row, count):
        def across(ref):
            return jnp.concatenate([ref[pl.ds(first_row + r, 1), :] for r in range(count)], axis=1)

        h = jnp.concatenate(
            [hx[pl.ds(first_row + r, K, stride=NH), :] for r in range(count)], axis=1
        )
        mean = jnp.sum(h, axis=0, keepdims=True) * (1.0 / K)
        anomaly = h - mean
        scaled = anomaly * (across(precision) * (1.0 / LEVELS))
        driven = scaled * (across(value) - mean)
        if banded:
            rows = [anomaly * turn(scaled, d) for d in range(K // 2 + 1)] + [driven]
        else:
            rows = [anomaly[q : q + 1, :] * scaled for q in range(K)] + [driven]
        for q in range(0, len(rows) // pair * pair, pair):
            hi, lo = split2(jnp.concatenate(rows[q : q + pair], axis=0))
            gmat[q * K : (q + pair) * K, :] = hi
            gmat[half_rows + q * K : half_rows + (q + pair) * K, :] = lo

    def against(span):
        g = gmat[...]
        if fused:
            return lax.dot_general(g, parts[:, span], NT, preferred_element_type=F32)
        return sum(
            lax.dot_general(g, parts[q * C : (q + 1) * C, span], NT, preferred_element_type=F32)
            for q in range(2)
        )

    def slab_sum(s, acc):
        fill(s * NB, NB)
        return acc + against(pl.ds(pl.multiple_of(s * nob, 128), nob))

    if S <= 4:
        fill(0, NH)
        total = against(slice(0, NOBS))
    else:
        total = jnp.zeros((2 * half_rows, 2 * C if fused else C), F32)
        total = lax.fori_loop(0, S, slab_sum, total)
    if fused:
        total = total[:, :C] + total[:, C:]
    if banded:
        total = total[:half_rows] + total[half_rows:]
        bands = [total[d * K : (d + 1) * K] for d in range(K // 2 + 2)]
        weights = transform_bands(bands[:-1], bands[-1], K)
    else:
        amat = total[:KK] + total[half_rows : half_rows + KK]
        drive = total[KK : KK + K] + total[half_rows + KK :]
        weights = transform_large(amat, drive, K, C, zr, yr, tr, ur)

    narrow = split2(jnp.concatenate(weights, axis=0))
    if fused:
        wide = jnp.dot(jnp.concatenate(narrow, axis=1), expand[...], preferred_element_type=F32)
    else:
        wide = sum(jnp.dot(v, expand[0:C, :], preferred_element_type=F32) for v in narrow)
    drain(block.at[0 : K - 1, 0 : 3 * RR], fwd_recv)
    states = [block[m] for m in range(K)]
    centre = sum(states) * (1.0 / K)
    spread = [v - centre for v in states]
    for a in range(3):
        for r in range(RR):
            row = a * RR + r
            z0 = (r // CHUNK_Y) * NZ
            acc = jnp.broadcast_to(centre[row : row + 1, :], (K, NZ))
            for m in range(K):
                acc = acc + spread[m][row : row + 1, :] * wide[m * K : (m + 1) * K, z0 : z0 + NZ]
            result[pl.ds(row, K, stride=RP), :] = acc

    def of(k):
        return pl.ds(pl.multiple_of(k * RP, 8), 3 * RR)

    for d in range(K - 1, 0, -1):
        copy(result.at[of(mate(d))], back.at[me, 0 : 3 * RR], ret_send, ret_recv, (mate(d), sl))
    back[me, 0 : 3 * RR] = result[of(me), :]
    drain(back.at[0 : K - 1, 0 : 3 * RR], ret_recv)
    for p in range(K):
        x, y0 = p // per_layer, (p % per_layer) * RR
        for a in range(3):
            out[0, a, x, y0 : y0 + RR, :] = back[p, a * RR : (a + 1) * RR, :]
    drain(halo, halo_send)
    drain(places.at[0 : S - 1], place_send)
    drain(early.at[0 : S - 1], early_send)
    drain(late.at[0 : S - 1], late_send)
    drain(hx.at[pl.ds(0, (K - 1) * NH)], hx_send)
    drain(block.at[0 : K - 1, 0 : 3 * RR], fwd_send)
    drain(back.at[0 : K - 1, 0 : 3 * RR], ret_send)


def solution(mesh):
    K, S = mesh.shape["member"], mesh.shape["space"]

    def shards(ensemble, obs_cell, obs_comp, obs_value, obs_precision, loc_obs, loc_level):
        CX, NY, NZ = ensemble.shape[2:]
        C = loc_obs.shape[0]
        NOBS = obs_value.shape[0]
        nob = obs_cell.shape[0]
        NB = nob // 128
        NH = NOBS // 128
        RR = CX * NY // K
        RP = -(-3 * RR // 8) * 8
        gram_rows = 2 * (K // 2 + 2) * K if K == 8 else 2 * (K * K + K)
        T = 2 * NB
        dims = (K, S, CX, NY, NZ, C, NOBS, RR, RP)
        large = (K, K, C) if K != 8 else (1, 8, 128)
        dma = pltpu.SemaphoreType.DMA
        vmem = pl.BlockSpec(memory_space=pltpu.VMEM)
        return pl.pallas_call(
            functools.partial(kernel, dims),
            out_shape=pltpu.VMEM(ensemble.shape, F32),
            in_specs=[pl.BlockSpec(memory_space=pl.ANY)] * 8,
            out_specs=vmem,
            scratch_shapes=[
                pltpu.VMEM(ensemble.shape, F32),
                pltpu.VMEM((1, nob), jnp.int32),
                pltpu.VMEM((NB, 128), jnp.int32),
                pltpu.VMEM((1, nob), jnp.int32),
                pltpu.VMEM((NH, 128), F32),
                pltpu.VMEM((NH, 128), F32),
                pltpu.VMEM((2, *loc_obs.shape), jnp.int32),
                dma((8,)),
                pltpu.VMEM((2, 3, CX, NY, NZ), F32),
                pltpu.VMEM((6, CX + 2, NY, NZ), F32),
                pltpu.VMEM((3, CX + 2, NY, NZ), F32),
                pltpu.VMEM((3 * CX * NY, NZ), F32),
                pltpu.VMEM((S, T, 128), F32),
                pltpu.VMEM((S, T, 128), jnp.int32),
                pltpu.VMEM((S, 2, T, 128), F32),
                pltpu.VMEM((K, RP, NZ), F32),
                pltpu.VMEM((K, RP, NZ), F32),
                pltpu.VMEM((K * NH, 128), F32),
                pltpu.VMEM((K * RP, NZ), F32),
                pltpu.VMEM((K, RP, NZ), F32),
                pltpu.VMEM((GROUP * NH, 128), F32),
                pltpu.VMEM((2 * C, NOBS), BF16),
                pltpu.VMEM((2 * NZ, nob), BF16),
                pltpu.VMEM((2 * C, RR // CHUNK_Y * NZ), BF16),
                pltpu.VMEM((gram_rows, NOBS if S <= 4 else nob), BF16),
                pltpu.VMEM(large, F32),
                pltpu.VMEM(large, F32),
                pltpu.VMEM(large, F32),
                pltpu.VMEM(large, F32),
            ] + [dma] * 14 + [pltpu.SemaphoreType.REGULAR] * 4,
            compiler_params=pltpu.CompilerParams(
                collective_id=0, has_side_effects=True, vmem_limit_bytes=60000 * 1024
            ),
            name="analysis_step",
        )(
            ensemble,
            obs_cell.reshape(1, nob),
            obs_cell.reshape(NB, 128),
            obs_comp.reshape(1, nob),
            obs_value.reshape(NH, 128),
            obs_precision.reshape(NH, 128),
            loc_obs,
            loc_level,
        )

    from jax.sharding import PartitionSpec as P

    field = P("member", None, "space", None, None)
    local = P(("space", "member"), None)
    return jax.shard_map(
        shards,
        mesh=mesh,
        in_specs=(field, P("space"), P("space"), P(), P(), local, local),
        out_specs=field,
        check_vma=False,
    )
```

```python
import functools

import jax
import jax.numpy as jnp
from jax import lax
from jax.experimental import pallas as pl
from jax.experimental.pallas import tpu as pltpu

NS_ITERS = 8
LEVELS = 8
CHUNK_Y = 3
CHUNK_Z = 4
GROUP = 16
PAIRS = ((0, 0), (1, 1), (2, 2), (0, 1), (0, 2), (1, 2))
WEIGHTS = (1.0, 1.0, 1.0, 2.0, 2.0, 2.0)
PLACE = {}
for _i, (_a, _b) in enumerate(PAIRS):
    PLACE[_a, _b] = PLACE[_b, _a] = _i
MESH = pl.DeviceIdType.MESH
F32 = jnp.float32
BF16 = jnp.bfloat16
NT = (((1,), (1,)), ((), ()))
TN = (((0,), (0,)), ((), ()))


def split2(x):
    hi = x.astype(BF16)
    return hi, (x - hi.astype(F32)).astype(BF16)


def split3(x):
    hi = x.astype(BF16)
    rest = x - hi.astype(F32)
    mid = rest.astype(BF16)
    low = (rest - mid.astype(F32)).astype(BF16)
    return hi, mid, low


def drain(ref, sem):
    pltpu.make_async_copy(ref, ref, sem).wait()


def gather_lanes(table, index):
    return jnp.take_along_axis(table, index, axis=1)


def dz(f):
    return pltpu.roll(f, f.shape[1] - 1, 1) - pltpu.roll(f, 1, 1)


def dy(f):
    n = f.shape[0]
    row = lax.broadcasted_iota(jnp.int32, f.shape, 0)
    after = jnp.where(row == n - 1, 0.0, pltpu.roll(f, n - 1, 0))
    before = jnp.where(row == 0, 0.0, pltpu.roll(f, 1, 0))
    return after - before


def filt(a, b, c):
    t = a + 2.0 * b + c
    return 0.0625 * (pltpu.roll(t, 1, 1) + 2.0 * t + pltpu.roll(t, t.shape[1] - 1, 1))


def strain(below, here, above):
    gx = [above[a] - below[a] for a in range(3)]
    gy = [dy(here[a]) for a in range(3)]
    gz = [dz(here[a]) for a in range(3)]
    rate = [
        0.5 * gx[0],
        0.5 * gy[1],
        0.5 * gz[2],
        0.25 * (gy[0] + gx[1]),
        0.25 * (gz[0] + gx[2]),
        0.25 * (gz[1] + gy[2]),
    ]
    diag = rate[0] * rate[0] + rate[1] * rate[1] + rate[2] * rate[2]
    off = rate[3] * rate[3] + rate[4] * rate[4] + rate[5] * rate[5]
    return rate, jnp.sqrt(2.0 * (diag + 2.0 * off))


def total_of(terms):
    while len(terms) > 1:
        terms = [
            terms[i] + terms[i + 1] if i + 1 < len(terms) else terms[i]
            for i in range(0, len(terms), 2)
        ]
    return terms[0]


def turn(v, d):
    k = v.shape[0]
    return pltpu.roll(v, (k - d) % k, 0) if d % k else v


def turned(bands, k):
    memo = {}

    def band(g, d):
        if (g, d) not in memo:
            memo[g, d] = turn(bands[g], d)
        return memo[g, d]

    def entry(f, d):
        f, d = f % k, d % k
        return band(f, d) if f <= k // 2 else band(k - f, (d + f) % k)

    return entry


def product(left, right, k):
    x, y = turned(left, k), turned(right, k)
    return [
        total_of([x(d, 0) * y(e - d, d) for d in range(k)]) for e in range(k // 2 + 1)
    ]


def transform_bands(bands, drive, k):
    half = k // 2
    matrix = [bands[0] + (k - 1) / 1.1] + bands[1:]
    squares = [v * v for v in matrix]
    off = total_of(squares[1:half])
    scale = jnp.sqrt(jnp.sum(squares[0] + squares[half] + 2.0 * off, axis=0, keepdims=True))
    inv_scale = 1.0 / scale
    root = [v * inv_scale for v in matrix]
    inverse = None
    for sweep in range(NS_ITERS):
        zy = product(inverse, root, k) if sweep else root
        factor = [1.5 - 0.5 * zy[0]] + [-0.5 * v for v in zy[1:]]
        if sweep < NS_ITERS - 1:
            root = product(factor, root, k)
        inverse = product(factor, inverse, k) if sweep else factor
    z = turned(inverse, k)

    def times(v):
        return total_of([z(d, 0) * turn(v, d) for d in range(k)])

    wbar = times(times(drive)) * inv_scale
    gain = jnp.sqrt(k - 1.0) / jnp.sqrt(scale)
    bent = [gain * z(d, 0) + turn(wbar, d) for d in range(k)]
    row = lax.broadcasted_iota(jnp.int32, wbar.shape, 0)
    out = []
    for m in range(k):
        v = bent[0]
        for d in range(1, k):
            v = jnp.where(row == (m - d) % k, bent[d], v)
        out.append(v)
    return out


def transform_large(amat, drive, k, cols, zr, yr, tr, ur):
    def each(fn):
        lax.fori_loop(0, k, lambda m, c: (fn(m), c)[1], 0)

    row = lax.broadcasted_iota(jnp.int32, (k, cols), 0)

    def eye(m):
        return jnp.where(row == m, 1.0, 0.0).astype(F32)

    def product(left, right, out, post):
        def one(m):
            def step(j, acc):
                return acc + left[m, pl.ds(j, 1), :] * right[j]

            out[m] = post(m, lax.fori_loop(0, k, step, jnp.zeros((k, cols), F32)))

        each(one)

    for m in range(k):
        yr[m] = amat[m * k : (m + 1) * k, :] + ((k - 1) / 1.1) * eye(m)
        zr[m] = eye(m)
    total = lax.fori_loop(0, k, lambda m, a: a + yr[m] * yr[m], jnp.zeros((k, cols), F32))
    scale = jnp.sqrt(jnp.sum(total, axis=0, keepdims=True))

    def shrink(m):
        yr[m] = yr[m] / scale

    each(shrink)

    def same(m, v):
        return v

    def copy(src, dst):
        def one(m):
            dst[m] = src[m]

        each(one)

    def sweep(i, c):
        product(zr, yr, tr, lambda m, v: 1.5 * eye(m) - 0.5 * v)
        product(yr, tr, ur, same)
        copy(ur, yr)
        product(tr, zr, ur, same)
        copy(ur, zr)
        return c

    lax.fori_loop(0, NS_ITERS, sweep, 0)
    product(zr, zr, ur, same)
    gain = jnp.sqrt(k - 1.0) / jnp.sqrt(scale)
    return [
        gain * zr[m] + jnp.sum(ur[m] * drive, axis=0, keepdims=True) / scale for m in range(k)
    ]


def kernel(
    dims,
    ens_hbm, cell_hbm, tile_hbm, comp_hbm, value_hbm, precision_hbm, loc_hbm, level_hbm, out,
    ens, cell, cells2, comp, value, precision, local, load_sem,
    halo, strided, smooth, flats, early, places, late, outbound, block, hx, result, back,
    hist, parts, pick, expand, gmat, zr, yr, tr, ur,
    halo_send, halo_recv, early_send, early_recv, place_send, place_recv,
    late_send, late_recv, hx_send, hx_recv, fwd_send, fwd_recv, ret_send, ret_recv, near_sem, mid_sem, far_sem, ready_sem,
):
    K, S, CX, NY, NZ, C, NOBS, RR, RP = dims
    me = lax.axis_index("member")
    sl = lax.axis_index("space")
    nob = NOBS // S
    NB = nob // 128
    NH = NOBS // 128
    R = 3 * CX * NY
    T = 2 * NB
    short = S == 4

    def mate(d):
        bit, to = 1, me
        while bit < K:
            if d // bit % 2:
                to = to + bit - 2 * bit * lax.rem(me // bit, 2)
            bit *= 2
        return to

    def space(d):
        return lax.rem(sl + d, S)

    barrier = pltpu.get_barrier_semaphore()
    mates = [(mate(a), sl) for a in range(K - 1, 0, -1)]
    columns = [(me, space(b)) for b in range(1, S)]

    def tell(sem, to):
        pl.semaphore_signal(sem, inc=1, device_id=to, device_id_type=MESH)

    if short:
        root = sl == 0

        @pl.when(root)
        def _():
            tell(barrier, (me, space(1)))
            tell(barrier, (me, space(S - 1)))
            for to in mates:
                tell(barrier, to)

        @pl.when(sl == 1)
        def _():
            tell(barrier, (me, space(1)))

        @pl.when(sl > 1)
        def _():
            tell(barrier, (me, space(S - 1)))

    else:
        for to in columns + mates:
            tell(barrier, to)
    if short:

        @pl.when(sl > 0)
        def _():
            pl.semaphore_wait(barrier, jnp.where(sl == S - 1, 1, 2))

        @pl.when(sl == 1)
        def _():
            tell(near_sem, (me, 0 * sl))

        @pl.when(sl == S - 2)
        def _():
            tell(mid_sem, (me, space(1)))

        @pl.when(sl == S - 1)
        def _():
            tell(far_sem, (me, 0 * sl))

    else:
        pl.semaphore_wait(barrier, S - 1 + len(mates))

    loads = [
        pltpu.make_async_copy(src, dst, load_sem.at[i])
        for i, (src, dst) in enumerate(
            ((cell_hbm, cell), (tile_hbm, cells2), (comp_hbm, comp), (ens_hbm, ens),
             (loc_hbm, local.at[0]), (level_hbm, local.at[1]), (value_hbm, value), (precision_hbm, precision))
        )
    ]
    for c in loads:
        c.start()

    def copy(src, dst, send, recv, to):
        pltpu.make_async_remote_copy(
            src_ref=src, dst_ref=dst, send_sem=send, recv_sem=recv, device_id=to, device_id_type=MESH
        ).start()

    def up(*at):
        copy(ens_hbm.at[0, *at], halo.at[0, *at], halo_send, halo_recv, (me, space(1)))

    def down():
        copy(ens_hbm.at[0], halo.at[1], halo_send, halo_recv, (me, space(S - 1)))

    if short:

        @pl.when(root)
        def _():
            pl.semaphore_wait(near_sem, 1)

            @pl.when(lax.rem(me, 2) == 0)
            def _():
                up(0)
                pl.semaphore_wait(far_sem, 1)
                down()
                up(slice(1, 3))

            @pl.when(lax.rem(me, 2) == 1)
            def _():
                up()
                pl.semaphore_wait(far_sem, 1)
                down()

        @pl.when(sl > 0)
        def _():
            up()

            @pl.when(sl == S - 1)
            def _():
                pl.semaphore_wait(mid_sem, 1)

            down()
    else:
        up()
        down()
    for c in loads:
        c.wait()

    row_t = lax.broadcasted_iota(jnp.int32, (T, 128), 0)
    lane_t = lax.broadcasted_iota(jnp.int32, (T, 128), 1)
    cells = cell[...]
    lanes = lax.rem(cells, NZ)
    levels = cells // NZ
    heights = lax.rem(levels, NY)
    rows = comp[...] * (CX * NY) + levels
    iota_lane = lax.broadcasted_iota(jnp.int32, (NZ, nob), 0)
    one_hot = jnp.where(iota_lane == lanes, 1.0, 0.0).astype(BF16)
    pick[0:NZ, :] = one_hot
    pick[NZ:, :] = one_hot
    eighth = lax.broadcasted_iota(jnp.int32, (8, nob), 0)
    here = rows - eighth
    after = jnp.where(heights == NY - 1, -R, rows + 1) - eighth
    before = jnp.where(heights == 0, -R, rows - 1) - eighth

    def of_lanes(field):
        return jnp.dot(
            jnp.concatenate(split2(field), axis=1), pick[...], preferred_element_type=F32
        )

    def of_rows(found, wanted):
        acc = jnp.zeros((8, nob), F32)
        for t in range(R // 8):
            acc = acc + jnp.where(wanted == 8 * t, found[8 * t : 8 * t + 8, :], 0.0)
        seen = jnp.sum(acc, axis=0, keepdims=True)
        return [seen[:, b * 128 : (b + 1) * 128] for b in range(NB)]

    def tile_of(values):
        tile = jnp.zeros((T, 128), F32)
        for r, v in enumerate(values):
            tile = jnp.where(row_t == r, v, tile)
        return tile

    at_cells = lax.rem(cells2[...] // NZ, NY)
    places[sl] = jnp.concatenate([at_cells, at_cells], axis=0)
    fields = jnp.concatenate([ens[0, a, x] for a in range(3) for x in range(CX)], axis=0)
    found = sum(
        jnp.dot(v, pick[0:NZ, :], preferred_element_type=F32) for v in split3(fields)
    )
    seen = of_rows(found, here)
    early[sl] = tile_of(seen + seen)

    iota_hi = lax.broadcasted_iota(jnp.int32, (NH, 128), 0)
    iota_lo = lax.broadcasted_iota(jnp.int32, (128, 128), 0)

    def group(g, carry):
        base = pl.multiple_of(g * GROUP, GROUP)
        index = local[0, pl.ds(base, GROUP), :]
        weight = local[1, pl.ds(base, GROUP), :].astype(F32)
        top = lax.shift_right_logical(index, 7)
        low = jnp.bitwise_and(index, 127)
        for j in range(GROUP):
            a = jnp.where(iota_hi == top[j : j + 1, :], weight[j : j + 1, :], 0.0).astype(BF16)
            b = jnp.where(iota_lo == low[j : j + 1, :], 1.0, 0.0).astype(BF16)
            hist[j * NH : (j + 1) * NH, :] = lax.dot_general(a, b, NT, preferred_element_type=F32)
        for h in range(NH):
            big, small = split2(hist[pl.ds(h, GROUP, stride=NH), :])
            parts[pl.ds(base, GROUP), h * 128 : (h + 1) * 128] = big
            parts[pl.ds(C + base, GROUP), h * 128 : (h + 1) * 128] = small
        return carry

    lax.fori_loop(0, C // GROUP, group, 0)

    blocks_z = NZ // CHUNK_Z
    groups = RR // CHUNK_Y
    looked_up = C == NZ and K == 8
    if not looked_up:
        ci = lax.broadcasted_iota(jnp.int32, (C, groups * NZ), 0)
        zi = lax.broadcasted_iota(jnp.int32, (C, groups * NZ), 1)
        spread_z = jnp.where(ci == zi // CHUNK_Z, 1.0, 0.0).astype(BF16)
        expand[0:C, :] = spread_z
        expand[C:, :] = spread_z

    if short:

        @pl.when(root)
        def _():
            pl.semaphore_wait(barrier, K - 1)
            for to in mates:
                tell(ready_sem, to)

    drain(halo, halo_recv)
    for d in range(1, S):
        copy(places.at[sl], places.at[sl], place_send, place_recv, (me, space(d)))
        copy(early.at[sl], early.at[sl], early_send, early_recv, (me, space(d)))

    def u(a, i):
        if i < 2:
            return halo[0, a, CX - 2 + i]
        if i < 2 + CX:
            return ens[0, a, i - 2]
        return halo[1, a, i - 2 - CX]

    mids = range(1, CX + 3)
    for i in mids:
        rate, size = strain(*[[u(a, i + s) for a in range(3)] for s in (-1, 0, 1)])
        for p in range(6):
            strided[p, i - 1] = size * rate[p]
    for x in range(CX):
        i = x + 2
        for a in range(3):
            px, pz = PLACE[a, 0], PLACE[a, 2]
            flats[(a * CX + x) * NY : (a * CX + x + 1) * NY, :] = (
                strided[px, i] - strided[px, i - 2] + dz(strided[pz, i - 1])
            )
    along_y = jnp.concatenate(
        [strided[PLACE[a, 1], x + 1] for a in range(3) for x in range(CX)], axis=0
    )
    found = of_lanes(flats[...])
    first = of_rows(found, here)
    found = of_lanes(along_y)
    first = first + of_rows(found, after)
    second = of_rows(found, before)
    for i in mids:
        for a in range(3):
            smooth[a, i - 1] = filt(u(a, i - 1), u(a, i), u(a, i + 1))
    numer = jnp.zeros((NY, NZ), F32)
    denom = jnp.zeros((NY, NZ), F32)
    for i in range(2, CX + 2):
        rate, size = strain(*[[smooth[a, i - 1 + s] for a in range(3)] for s in (-1, 0, 1)])
        for p, (a, b) in enumerate(PAIRS):
            prod = filt(*[u(a, i + s) * u(b, i + s) for s in (-1, 0, 1)])
            leonard = prod - smooth[a, i - 1] * smooth[b, i - 1]
            model = 2.0 * (
                filt(strided[p, i - 2], strided[p, i - 1], strided[p, i]) - 4.0 * size * rate[p]
            )
            numer = numer + WEIGHTS[p] * (leonard * model)
            denom = denom + WEIGHTS[p] * (model * model)
    tiles = NY // 8
    row_8 = lax.broadcasted_iota(jnp.int32, (8, 128), 0)
    lane_8 = lax.broadcasted_iota(jnp.int32, (8, 128), 1)
    planes = []
    for v in (numer, denom):
        packed = jnp.zeros((8, 128), F32)
        for j in range(tiles):
            total = jnp.sum(v[j * 8 : j * 8 + 8], axis=1, keepdims=True)
            packed = jnp.where(lane_8 == j, total, packed)
        packed = gather_lanes(packed, lane_8 // 8)
        packed = jnp.where(lax.rem(lane_8, 8) == row_8, packed, 0.0)
        planes.append(jnp.sum(packed, axis=0, keepdims=True))
    late[sl, 0] = tile_of(first)
    late[sl, 1] = tile_of(second + planes)
    if short:

        @pl.when(root)
        def _():
            pl.semaphore_wait(ready_sem, K - 1)

    for d in range(1, S):
        copy(late.at[sl], late.at[sl], late_send, late_recv, (me, space(d)))

    drain(early.at[0 : S - 1], early_recv)
    drain(places.at[0 : S - 1], place_recv)
    drain(late.at[0 : S - 1], late_recv)

    count = float(CX * S * NZ)
    above, below = [
        sum(jnp.broadcast_to(late[s, 1, NB + q : NB + q + 1, :], (T, 128)) for s in range(S))
        for q in range(2)
    ]
    ratio = jnp.where(lane_t < NY, (above / count) / (below / count + 1e-06), 0.0)
    quarter = 0.25 * ratio
    values = []
    for s in range(S):
        y = places[s]
        ya = jnp.where(row_t < NB, y, y + 1)
        yb = jnp.maximum(y - 1, 0)
        v = late[s, 0] * gather_lanes(quarter, ya)
        v = v - jnp.where(row_t < NB, late[s, 1] * gather_lanes(quarter, yb), 0.0)
        values.append(v + pltpu.roll(v, NB, 0) + early[s])
    own = pl.ds(pl.multiple_of(me * NH, 8), NH)
    hx[own, :] = jnp.concatenate(
        [jnp.where(row_t < NB, values[s], values[s + 1]) for s in range(0, S, 2)], axis=0
    )
    for d in range(1, K):
        copy(hx.at[own], hx.at[own], hx_send, hx_recv, (mate(d), sl))

    coeff = jnp.concatenate(
        [gather_lanes(ratio[0:8], 8 * j + row_8) for j in range(tiles)], axis=0
    )
    per_layer = NY // RR
    for x in range(CX):
        for a in range(3):
            flat = flats[(a * CX + x) * NY : (a * CX + x + 1) * NY, :]
            term = coeff * flat + dy(coeff * strided[PLACE[a, 1], x + 1])
            f = ens[0, a, x] + 0.25 * term
            for t in range(per_layer):
                p = x * per_layer + t
                outbound[p, a * RR : (a + 1) * RR, :] = f[t * RR : (t + 1) * RR, :]
    for d in range(1, K):
        copy(outbound.at[mate(d), 0 : 3 * RR], block.at[me, 0 : 3 * RR], fwd_send, fwd_recv, (mate(d), sl))
    block[me] = outbound[me]

    drain(hx.at[pl.ds(0, (K - 1) * NH)], hx_recv)

    KK = K * K
    pair = max(1, 16 // K)
    banded = K == 8
    half_rows = (K // 2 + 2) * K if banded else KK + K
    assert half_rows // K % pair == 0
    fused = C % 128 == 0

    def fill(first_row, count):
        def across(ref):
            return jnp.concatenate([ref[pl.ds(first_row + r, 1), :] for r in range(count)], axis=1)

        h = jnp.concatenate(
            [hx[pl.ds(first_row + r, K, stride=NH), :] for r in range(count)], axis=1
        )
        mean = jnp.sum(h, axis=0, keepdims=True) * (1.0 / K)
        anomaly = h - mean
        scaled = anomaly * (across(precision) * (1.0 / LEVELS))
        driven = scaled * (across(value) - mean)
        if banded:
            rows = [anomaly * turn(scaled, d) for d in range(K // 2 + 1)] + [driven]
        else:
            rows = [anomaly[q : q + 1, :] * scaled for q in range(K)] + [driven]
        for q in range(0, len(rows) // pair * pair, pair):
            hi, lo = split2(jnp.concatenate(rows[q : q + pair], axis=0))
            gmat[q * K : (q + pair) * K, :] = hi
            gmat[half_rows + q * K : half_rows + (q + pair) * K, :] = lo

    def against(span):
        g = gmat[...]
        if fused:
            return lax.dot_general(g, parts[:, span], NT, preferred_element_type=F32)
        return sum(
            lax.dot_general(g, parts[q * C : (q + 1) * C, span], NT, preferred_element_type=F32)
            for q in range(2)
        )

    def slab_sum(s, acc):
        fill(s * NB, NB)
        return acc + against(pl.ds(pl.multiple_of(s * nob, 128), nob))

    if S <= 4:
        fill(0, NH)
        total = against(slice(0, NOBS))
    else:
        total = jnp.zeros((2 * half_rows, 2 * C if fused else C), F32)
        total = lax.fori_loop(0, S, slab_sum, total)
    if fused:
        total = total[:, :C] + total[:, C:]
    if banded:
        total = total[:half_rows] + total[half_rows:]
        bands = [total[d * K : (d + 1) * K] for d in range(K // 2 + 2)]
        weights = transform_bands(bands[:-1], bands[-1], K)
    else:
        amat = total[:KK] + total[half_rows : half_rows + KK]
        drive = total[KK : KK + K] + total[half_rows + KK :]
        weights = transform_large(amat, drive, K, C, zr, yr, tr, ur)

    if looked_up:
        lane = lax.broadcasted_iota(jnp.int32, (K, C), 1) // CHUNK_Z
        wide = [[gather_lanes(w, lane + g * blocks_z) for w in weights] for g in range(groups)]
    else:
        narrow = split2(jnp.concatenate(weights, axis=0))
        if fused:
            spread_w = jnp.dot(
                jnp.concatenate(narrow, axis=1), expand[...], preferred_element_type=F32
            )
        else:
            spread_w = sum(
                jnp.dot(v, expand[0:C, :], preferred_element_type=F32) for v in narrow
            )
        wide = [
            [spread_w[m * K : (m + 1) * K, g * NZ : (g + 1) * NZ] for m in range(K)]
            for g in range(groups)
        ]
    drain(block.at[0 : K - 1, 0 : 3 * RR], fwd_recv)
    states = [block[m] for m in range(K)]
    centre = sum(states) * (1.0 / K)
    spread = [v - centre for v in states]
    for g in range(groups):
        for a in range(3):
            for r in range(g * CHUNK_Y, (g + 1) * CHUNK_Y):
                row = a * RR + r
                acc = jnp.broadcast_to(centre[row : row + 1, :], (K, NZ))
                for m in range(K):
                    acc = acc + spread[m][row : row + 1, :] * wide[g][m]
                result[pl.ds(row, K, stride=RP), :] = acc

    def of(k):
        return pl.ds(pl.multiple_of(k * RP, 8), 3 * RR)

    for d in range(1, K):
        copy(result.at[of(mate(d))], back.at[me, 0 : 3 * RR], ret_send, ret_recv, (mate(d), sl))
    back[me, 0 : 3 * RR] = result[of(me), :]
    drain(back.at[0 : K - 1, 0 : 3 * RR], ret_recv)
    for p in range(K):
        x, y0 = p // per_layer, (p % per_layer) * RR
        for a in range(3):
            out[0, a, x, y0 : y0 + RR, :] = back[p, a * RR : (a + 1) * RR, :]
    drain(halo, halo_send)
    drain(places.at[0 : S - 1], place_send)
    drain(early.at[0 : S - 1], early_send)
    drain(late.at[0 : S - 1], late_send)
    drain(hx.at[pl.ds(0, (K - 1) * NH)], hx_send)
    drain(block.at[0 : K - 1, 0 : 3 * RR], fwd_send)
    drain(back.at[0 : K - 1, 0 : 3 * RR], ret_send)


def solution(mesh):
    K, S = mesh.shape["member"], mesh.shape["space"]

    def shards(ensemble, obs_cell, obs_comp, obs_value, obs_precision, loc_obs, loc_level):
        CX, NY, NZ = ensemble.shape[2:]
        C = loc_obs.shape[0]
        NOBS = obs_value.shape[0]
        nob = obs_cell.shape[0]
        NB = nob // 128
        NH = NOBS // 128
        RR = CX * NY // K
        RP = -(-3 * RR // 8) * 8
        gram_rows = 2 * (K // 2 + 2) * K if K == 8 else 2 * (K * K + K)
        T = 2 * NB
        dims = (K, S, CX, NY, NZ, C, NOBS, RR, RP)
        large = (K, K, C) if K != 8 else (1, 8, 128)
        dma = pltpu.SemaphoreType.DMA
        vmem = pl.BlockSpec(memory_space=pltpu.VMEM)
        return pl.pallas_call(
            functools.partial(kernel, dims),
            out_shape=pltpu.VMEM(ensemble.shape, F32),
            in_specs=[pl.BlockSpec(memory_space=pl.ANY)] * 8,
            out_specs=vmem,
            scratch_shapes=[
                pltpu.VMEM(ensemble.shape, F32),
                pltpu.VMEM((1, nob), jnp.int32),
                pltpu.VMEM((NB, 128), jnp.int32),
                pltpu.VMEM((1, nob), jnp.int32),
                pltpu.VMEM((NH, 128), F32),
                pltpu.VMEM((NH, 128), F32),
                pltpu.VMEM((2, *loc_obs.shape), jnp.int32),
                dma((8,)),
                pltpu.VMEM((2, 3, CX, NY, NZ), F32),
                pltpu.VMEM((6, CX + 2, NY, NZ), F32),
                pltpu.VMEM((3, CX + 2, NY, NZ), F32),
                pltpu.VMEM((3 * CX * NY, NZ), F32),
                pltpu.VMEM((S, T, 128), F32),
                pltpu.VMEM((S, T, 128), jnp.int32),
                pltpu.VMEM((S, 2, T, 128), F32),
                pltpu.VMEM((K, RP, NZ), F32),
                pltpu.VMEM((K, RP, NZ), F32),
                pltpu.VMEM((K * NH, 128), F32),
                pltpu.VMEM((K * RP, NZ), F32),
                pltpu.VMEM((K, RP, NZ), F32),
                pltpu.VMEM((GROUP * NH, 128), F32),
                pltpu.VMEM((2 * C, NOBS), BF16),
                pltpu.VMEM((2 * NZ, nob), BF16),
                pltpu.VMEM((2 * C, RR // CHUNK_Y * NZ), BF16),
                pltpu.VMEM((gram_rows, NOBS if S <= 4 else nob), BF16),
                pltpu.VMEM(large, F32),
                pltpu.VMEM(large, F32),
                pltpu.VMEM(large, F32),
                pltpu.VMEM(large, F32),
            ] + [dma] * 14 + [pltpu.SemaphoreType.REGULAR] * 4,
            compiler_params=pltpu.CompilerParams(
                collective_id=0, has_side_effects=True, vmem_limit_bytes=60000 * 1024
            ),
            name="analysis_step",
        )(
            ensemble,
            obs_cell.reshape(1, nob),
            obs_cell.reshape(NB, 128),
            obs_comp.reshape(1, nob),
            obs_value.reshape(NH, 128),
            obs_precision.reshape(NH, 128),
            loc_obs,
            loc_level,
        )

    from jax.sharding import PartitionSpec as P

    field = P("member", None, "space", None, None)
    local = P(("space", "member"), None)
    return jax.shard_map(
        shards,
        mesh=mesh,
        in_specs=(field, P("space"), P("space"), P(), P(), local, local),
        out_specs=field,
        check_vma=False,
    )
```
